32 devices in a mesh: ta: 4 (over z), gz: 4 (over x, core), xy: 2 (over y).
Axes of the slice: x: 2, y: 2, z: 4, core: 2. Of those that a mesh axis runs over, the one named last changes fastest.
Arguments:
- links: float32 [4, 2, 3, 3, 4, 8, 512], P(None, None, None, None, 'ta', 'xy', 'gz'), may hold values from -0.72 to 1.72
- guess: float32 [12, 2, 4, 3, 4, 8, 512], P(None, None, None, None, 'ta', 'xy', 'gz'), may hold values from -1.5 to 1.5
- source_sites: int32 [4, 2, 4, 4], P('ta', 'xy', 'gz'), may hold values from 0 to 31, as said below
Outputs:
- solution: float32 [12, 2, 4, 3, 4, 8, 512], P(None, None, None, None, 'ta', 'xy', 'gz')
- residual: float32 [12, 2, 4, 3, 4, 8, 512], P(None, None, None, None, 'ta', 'xy', 'gz')
The draws below stay inside these ranges and needn't reach their ends.
Inputs may be any that keep to these rules, and one draw needn't show every extreme that they name: `source_sites`: each entry is an offset inside its block: time below 1, y below 4, z below 4, x below 32.
All inputs are finite; a program needn't handle non-finite values.
Results may differ from the reference program's by a relative error of at most 0.00012.
Values sent between devices are 32-bit elements; how exact they have to be, the bound alone decides.
A program may use at most 128 MiB of HBM per device.

```python
import math
import jax
import jax.numpy as jnp
import numpy as np
from jax import lax

LT = 1
LY = 4
LZ = 4
LX = 32
NSMEAR = 8
NT = 4
NY = 8
NZ = 16


def draw_links(key, part):
    full_shape = (4, 2, 3, 3, NT, NY, NZ * LX)
    noise = 0.18 * jnp.clip(jax.random.normal(key, full_shape), -4.0, 4.0)
    identity = jnp.eye(3, dtype=jnp.float32)
    unit = jnp.stack([identity, jnp.zeros_like(identity)], axis=0)
    return (unit[None, :, :, :, None, None, None] + noise).astype(jnp.float32)


def draw_guess(key, part):
    main_key, slice_key = jax.random.split(key)
    full_shape = (12, 2, 4, 3, NT, NY, NZ * LX)
    rising = 10.0 ** (jnp.arange(NT, dtype=jnp.float32) / NT)
    slices = jax.random.uniform(slice_key, (NZ,), minval=0.0, maxval=math.log(3.0))
    slice_scale = jnp.repeat(jnp.exp(slices), LX)
    noise = jnp.clip(jax.random.normal(main_key, full_shape), -5.0, 5.0)
    return (0.01 * noise * rising[:, None, None] * slice_scale).astype(jnp.float32)


def draw_source_sites(key, part):
    blocks = (NT // LT, NY // LY, NZ // LZ)
    subkeys = jax.random.split(key, 4)
    limits = (LT, LY, LZ, LX)
    columns = [jax.random.randint(subkeys[position], blocks, 0, limits[position]) for position in range(4)]
    return jnp.stack(columns, axis=-1).astype(jnp.int32)


def setup_inputs(seed: int = 0) -> dict:
    arg_keys = jax.random.split(jax.random.key(seed), 4)
    links = draw_links(jax.random.fold_in(arg_keys[3], 71), 0)
    guess = draw_guess(jax.random.fold_in(arg_keys[3], 71), 0)
    source_sites = draw_source_sites(jax.random.fold_in(arg_keys[3], 71), 0)
    return dict(links=links, guess=guess, source_sites=source_sites)


HIGHEST = lax.Precision.HIGHEST
hopping = 0.12
smear_weight = 0.25
smear_norm = 2.0


def pauli_blocks():
    sigma_one = np.array([[0, 1], [1, 0]], dtype=complex)
    sigma_two = np.array([[0, -1j], [1j, 0]], dtype=complex)
    sigma_three = np.array([[1, 0], [0, -1]], dtype=complex)
    return [-1j * sigma_one, -1j * sigma_two, -1j * sigma_three, np.eye(2, dtype=complex)]


def real_form(matrix):
    upper = np.concatenate([matrix.real, -matrix.imag], axis=1)
    lower = np.concatenate([matrix.imag, matrix.real], axis=1)
    return np.concatenate([upper, lower], axis=0).astype(np.float32)


def full_table(direction, parity):
    block_matrix = pauli_blocks()[direction]
    project_rows = np.concatenate([np.eye(2), parity * block_matrix], axis=1)
    lift_rows = np.concatenate([np.eye(2), parity * block_matrix.conj().T], axis=0)
    return real_form(lift_rows @ project_rows)


def spin_apply(matrix, field):
    spin_table = jnp.asarray(matrix)
    copies = field.shape[0]
    flattened = field.reshape((copies, spin_table.shape[1]) + field.shape[3:])
    applied = jnp.einsum('ij,rjatyw->riatyw', spin_table, flattened, precision=HIGHEST)
    return applied.reshape((copies, 2, spin_table.shape[0] // 2) + field.shape[3:])


def colour_times(link, field, adjoint):
    form = 'batyw,...btyw->...atyw' if adjoint else 'abtyw,...btyw->...atyw'
    parity = -1.0 if adjoint else 1.0
    real_part = field[:, 0]
    imag_part = field[:, 1]
    out_real = jnp.einsum(form, link[0], real_part, precision=HIGHEST) - parity * jnp.einsum(form, link[1], imag_part, precision=HIGHEST)
    out_imag = jnp.einsum(form, link[0], imag_part, precision=HIGHEST) + parity * jnp.einsum(form, link[1], real_part, precision=HIGHEST)
    return jnp.stack([out_real, out_imag], axis=1)


def roll_x(field, amount):
    shaped = field.reshape(field.shape[:-1] + (field.shape[-1] // LX, LX))
    return jnp.roll(shaped, amount, axis=-1).reshape(field.shape)


def shift_ahead(field, direction):
    if direction == 0:
        return roll_x(field, -1)
    if direction == 1:
        return jnp.roll(field, -1, axis=-2)
    if direction == 2:
        return jnp.roll(field, -LX, axis=-1)
    return jnp.roll(field, -1, axis=-3)


def shift_behind(field, direction):
    if direction == 0:
        return roll_x(field, 1)
    if direction == 1:
        return jnp.roll(field, 1, axis=-2)
    if direction == 2:
        return jnp.roll(field, LX, axis=-1)
    return jnp.roll(field, 1, axis=-3)


def point_sources(source_sites):
    time_ids = jnp.arange(NT, dtype=jnp.int32)
    row_ids = jnp.arange(NY, dtype=jnp.int32)
    slice_ids = jnp.arange(NZ, dtype=jnp.int32)
    column_ids = jnp.arange(LX, dtype=jnp.int32)
    offsets = source_sites[(time_ids // LT)[:, None, None], (row_ids // LY)[None, :, None], (slice_ids // LZ)[None, None, :]]
    site_hit = (offsets[..., 0] == (time_ids % LT)[:, None, None]) & (offsets[..., 1] == (row_ids % LY)[None, :, None]) & (offsets[..., 2] == (slice_ids % LZ)[None, None, :])
    site_hit = site_hit[..., None] & (offsets[..., 3:4] == column_ids)
    mask = jnp.where(site_hit, 1.0, 0.0).astype(jnp.float32).reshape(NT, NY, NZ * LX)
    identity = jnp.eye(3, dtype=jnp.float32)
    real_part = identity[:, :, None, None, None] * mask
    return jnp.stack([real_part, jnp.zeros_like(real_part)], axis=1)


def smear_step(colour_field, links):
    total = jnp.zeros_like(colour_field)
    for direction in range(3):
        link = links[direction]
        ahead_part = colour_times(link, shift_ahead(colour_field, direction), False)
        behind_part = shift_behind(colour_times(link, colour_field, True), direction)
        total = total + ahead_part + behind_part
    return (colour_field + smear_weight * total) / smear_norm


def spread(colour_field):
    identity = jnp.eye(4, dtype=jnp.float32)
    grown = identity[:, None, None, :, None, None, None, None] * colour_field[None, :, :, None, :, :, :, :]
    return grown.reshape((12, 2, 4, 3) + colour_field.shape[3:])


def wilson_single(field, links):
    time_ids = jnp.arange(NT, dtype=jnp.int32)
    ahead_parity = jnp.where(time_ids == NT - 1, -1.0, 1.0).astype(jnp.float32)[:, None, None]
    behind_parity = jnp.where(time_ids == 0, -1.0, 1.0).astype(jnp.float32)[:, None, None]
    total = jnp.zeros_like(field)
    for direction in range(4):
        link = links[direction]
        ahead_part = shift_ahead(field, direction)
        behind_part = shift_behind(colour_times(link, field, True), direction)
        if direction == 3:
            ahead_part = ahead_part * ahead_parity
            behind_part = behind_part * behind_parity
        ahead_part = colour_times(link, ahead_part, False)
        total = total + spin_apply(full_table(direction, -1.0), ahead_part) + spin_apply(full_table(direction, 1.0), behind_part)
    return field - hopping * total


def wilson(field, links):
    return lax.map(lambda single: wilson_single(single[None], links)[0], field)


def dagger(field, links):
    chirality = jnp.array([1.0, 1.0, -1.0, -1.0], dtype=jnp.float32)[None, None, :, None, None, None, None]
    return chirality * wilson(chirality * field, links)


def reference(links, guess, source_sites):
    colour_field = point_sources(source_sites)
    for iteration in range(NSMEAR):
        colour_field = smear_step(colour_field, links)
    right_side = spread(colour_field)
    defect = right_side - wilson(guess, links)
    search = dagger(defect, links)
    applied = wilson(search, links)
    summed_axes = (1, 2, 3, 4, 5, 6)
    norm_now = jnp.sum(search * search, axis=summed_axes)
    curvature = jnp.sum(applied * applied, axis=summed_axes)
    step_length = (norm_now / curvature)[:, None, None, None, None, None, None]
    solution = guess + step_length * search
    residual = search - step_length * dagger(applied, links)
    return solution, residual
```

```python
import functools

import jax
import jax.numpy as jnp
from jax import lax
from jax.experimental import pallas as pl
from jax.experimental.pallas import tpu as pltpu
from jax.sharding import PartitionSpec as P

LX = 32
NSMEAR = 8
HOP = 0.12
PAIRS = 6
EDGE_CHUNK = 3
EARLY = 4
TIME_CHUNK = 1
MESH = pl.DeviceIdType.MESH
AXES = ("xy", "gz", "ta")

E_ROWS = (
    ((1, -1j), (0, -1j)),
    ((1, -1), (0, 1)),
    ((0, -1j), (1, 1j)),
    ((0, 1), (1, 1)),
)


def times(coef, z):
    re, im = z
    if coef == 1:
        return (1, re), (1, im)
    if coef == -1:
        return (-1, re), (-1, im)
    if coef == 1j:
        return (-1, im), (1, re)
    return (1, im), (-1, re)


def add_term(z, coef, other):
    out = []
    for base, (sign, term) in zip(z, times(coef, other)):
        out.append(base + term if sign > 0 else base - term)
    return tuple(out)


def project(f, mu, parity):
    half = []
    for row in range(2):
        column, coef = E_ROWS[mu][row]
        half.append([add_term(f[row][a], parity * coef, f[2 + column][a]) for a in range(3)])
    return half


def lift_add(total, h, mu, parity):
    for row in range(2):
        column, coef = E_ROWS[mu][row]
        for a in range(3):
            total[row][a] = add_term(total[row][a], 1, h[row][a])
            low = parity * complex(coef).conjugate()
            total[2 + column][a] = add_term(total[2 + column][a], low, h[row][a])


def link_times(link, mu, vectors, adjoint):
    def entry(a, b):
        if adjoint:
            a, b = b, a
        base = mu * 18 + a * 3 + b
        return link[base], link[base + 9]

    out = [[None] * 3 for _ in vectors]
    for a in range(3):
        totals = [None] * len(vectors)
        for b in range(3):
            ur, ui = entry(a, b)
            for k, vec in enumerate(vectors):
                re, im = vec[b]
                if adjoint:
                    tr, ti = ur * re + ui * im, ur * im - ui * re
                else:
                    tr, ti = ur * re - ui * im, ur * im + ui * re
                old = totals[k]
                totals[k] = (tr, ti) if old is None else (old[0] + tr, old[1] + ti)
        for k in range(len(vectors)):
            out[k][a] = totals[k]
    return out


def flat(vectors):
    return [vec[a][part] for part in range(2) for vec in vectors for a in range(3)]


def unflat(items, count):
    return [
        [(items[k * 3 + a], items[3 * count + k * 3 + a]) for a in range(3)] for k in range(count)
    ]


class Shifts:
    def __init__(self):
        row = lax.broadcasted_iota(jnp.int32, (8, 128), 0)
        lane = lax.broadcasted_iota(jnp.int32, (8, 128), 1)
        self.low = row < 4
        self.lane = lane
        self.place = ([row % 4 == k for k in range(4)], [lane // LX == k for k in range(4)])
        self.x_first = lane % LX == 0
        self.x_last = lane % LX == LX - 1
        self.unit = ((0, 1, 8), (1, LX, 128))

    def roll(self, v, kind, steps):
        axis, unit, size = self.unit[kind]
        amount = (steps * unit) % size
        return v if amount == 0 else pltpu.roll(v, amount, axis)

    def pack(self, items, kind, ahead):
        packed = []
        for g in range(0, len(items), 4):
            out = None
            for k in range(4):
                v = self.roll(items[g + k], kind, k if ahead else k - 3)
                out = v if out is None else jnp.where(self.place[kind][k], v, out)
            packed.append(out)
        return packed

    def shift(self, items, packed, kind, ahead):
        outs = []
        for i, v in enumerate(items):
            got = packed[i // 4]
            k = i % 4
            if ahead:
                moved = self.roll(v, kind, -1)
                outs.append(jnp.where(self.place[kind][3], self.roll(got, kind, 3 - k), moved))
            else:
                moved = self.roll(v, kind, 1)
                outs.append(jnp.where(self.place[kind][0], self.roll(got, kind, -k), moved))
        return outs

    def along_x(self, items, ahead):
        outs = []
        for v in items:
            if ahead:
                a, b = pltpu.roll(v, 127, 1), pltpu.roll(v, LX - 1, 1)
                outs.append(jnp.where(self.x_last, b, a))
            else:
                a, b = pltpu.roll(v, 1, 1), pltpu.roll(v, 129 - LX, 1)
                outs.append(jnp.where(self.x_first, b, a))
        return outs


def kernel(
    sizes, sites_hbm, links_hbm, guess_hbm, sol_ref, res_ref,
    sites_ref, links_ref, guess_ref,
    link, guess, field_a, field_b, search, acc, right, carried,
    edge_out, edge_in, time_out, time_in, sm_out, sm_in, smt_out, smt_in,
    red_out, red_in, sums, hops,
    load_sem, edge_sem, time_sem, sm_sem, smt_sem, red_sem, send_sem,
):
    loads = [
        pltpu.make_async_copy(src, dst, load_sem.at[k])
        for k, (src, dst) in enumerate(
            ((links_hbm, links_ref), (sites_hbm, sites_ref), (guess_hbm, guess_ref))
        )
    ]
    for load in loads:
        load.start()

    n_of = dict(zip(AXES, sizes))
    me = {axis: lax.axis_index(axis) for axis in AXES}

    def peer(axis, step):
        return {axis: lax.rem(me[axis] + step + n_of[axis], n_of[axis])}

    barrier = pltpu.get_barrier_semaphore()
    for axis in AXES:
        for k in range(1, n_of[axis]):
            pl.semaphore_signal(barrier, inc=1, device_id=peer(axis, k), device_id_type=MESH)

    sh = Shifts()

    loads[0].wait()
    sign = jnp.where(me["ta"] == n_of["ta"] - 1, -1.0, 1.0).astype(jnp.float32)
    for i in range(72):
        v = links_ref[i]
        if i >= 54:
            v = v * sign
        link[i, 0:4, :] = v
        link[i, 4:8, :] = v

    def rhs_of(p):
        first = jnp.where(p < 4, 3 * p, 6 * p - 22)
        second = jnp.where(p < 4, 3 * p + 1, 6 * p - 19)
        return first, second

    def load_guess(p, _):
        first, second = rhs_of(p)
        for i in range(24):
            guess[p, i, 0:4, :] = guess_ref[first, i]
            guess[p, i, 4:8, :] = guess_ref[second, i]
        return _

    loads[1].wait()
    loads[2].wait()
    lax.fori_loop(0, PAIRS, load_guess, 0)
    pl.semaphore_wait(barrier, sum(n - 1 for n in sizes))

    def part_of(p, chunk):
        return pl.ds(p, chunk)

    def start_last(make, w, d, p, chunk):
        if chunk == 1:
            make(w, d, p).start()
        else:
            @pl.when(lax.rem(p, chunk) == chunk - 1)
            def _():
                make(w, d, p - (chunk - 1)).start()

    def await_first(make, w, p, chunk, dirs):
        def wait():
            for d in dirs:
                make(w, d, p).wait_recv()
        if chunk == 1:
            wait()
        else:
            pl.when(lax.rem(p, chunk) == 0)(wait)

    def edge_copy(w, d, p):
        axis, step = (("xy", -1), ("xy", 1), ("gz", -1), ("gz", 1))[d]
        return pltpu.make_async_remote_copy(
            src_ref=edge_out.at[w, d, part_of(p, EDGE_CHUNK)], dst_ref=edge_in.at[w, d, part_of(p, EDGE_CHUNK)],
            send_sem=send_sem.at[0], recv_sem=edge_sem.at[lax.rem(w, 2), d, p // EDGE_CHUNK],
            device_id=peer(axis, step), device_id_type=MESH,
        )

    def time_copy(w, d, p):
        return pltpu.make_async_remote_copy(
            src_ref=time_out.at[w, d, part_of(p, TIME_CHUNK)], dst_ref=time_in.at[w, d, part_of(p, TIME_CHUNK)],
            send_sem=send_sem.at[1], recv_sem=time_sem.at[lax.rem(w, 2), d, p],
            device_id=peer("ta", (-1, 1)[d]), device_id_type=MESH,
        )

    def load_field(ref, p):
        return unflat([ref[p, i] for i in range(24)], 4)

    def send_time(f, w, p, par, held=False):
        def start(d):
            if held:
                pl.when(p < PAIRS - 1)(lambda: time_copy(w, d, p).start())
            else:
                time_copy(w, d, p).start()

        for i, v in enumerate(flat(project(f, 3, -par))):
            time_out[w, 0, p, i] = v
        start(0)
        for i, v in enumerate(flat(link_times(link, 3, project(f, 3, par), True))):
            time_out[w, 1, p, i] = v
        start(1)

    def send_edges(f, w, p, par):
        for kind, mu in ((0, 1), (1, 2)):
            for i, v in enumerate(sh.pack(flat(project(f, mu, -par)), kind, True)):
                edge_out[w, 2 * kind, p, i] = v
            start_last(edge_copy, w, 2 * kind, p, EDGE_CHUNK)
            behind = flat(link_times(link, mu, project(f, mu, par), True))
            for i, v in enumerate(behind):
                carried[kind, p, i] = v
            for i, v in enumerate(sh.pack(behind, kind, False)):
                edge_out[w, 2 * kind + 1, p, i] = v
            start_last(edge_copy, w, 2 * kind + 1, p, EDGE_CHUNK)

    def interior(src, par, first=0, end=PAIRS):
        def body(p, _):
            f = load_field(src, p)
            zero = jnp.zeros((8, 128), jnp.float32)
            total = [[(zero, zero)] * 3 for _ in range(4)]
            ahead = unflat(sh.along_x(flat(project(f, 0, -par)), True), 2)
            lift_add(total, link_times(link, 0, ahead, False), 0, -par)
            behind = flat(link_times(link, 0, project(f, 0, par), True))
            lift_add(total, unflat(sh.along_x(behind, False), 2), 0, par)
            for i, v in enumerate(flat(total)):
                acc[p, i] = v
            return _
        lax.fori_loop(first, end, body, 0)

    def receive_body(src, w, p, par):
        await_first(edge_copy, w, p, EDGE_CHUNK, range(4))
        await_first(time_copy, w, p, TIME_CHUNK, range(2))
        f = load_field(src, p)
        total = load_field(acc, p)
        for kind, mu in ((0, 1), (1, 2)):
            got = [edge_in[w, 2 * kind, p, i] for i in range(3)]
            ahead = unflat(sh.shift(flat(project(f, mu, -par)), got, kind, True), 2)
            lift_add(total, link_times(link, mu, ahead, False), mu, -par)
            got = [edge_in[w, 2 * kind + 1, p, i] for i in range(3)]
            local = [carried[kind, p, i] for i in range(12)]
            lift_add(total, unflat(sh.shift(local, got, kind, False), 2), mu, par)
        ahead = unflat([time_in[w, 0, p, i] for i in range(12)], 2)
        lift_add(total, link_times(link, 3, ahead, False), 3, -par)
        lift_add(total, unflat([time_in[w, 1, p, i] for i in range(12)], 2), 3, par)
        return [a - HOP * b for a, b in zip(flat(f), flat(total))]

    def sm_copy(step, d):
        axis, hop = (("xy", -1), ("xy", 1), ("gz", -1), ("gz", 1))[d]
        return pltpu.make_async_remote_copy(
            src_ref=sm_out.at[step, d], dst_ref=sm_in.at[step, d],
            send_sem=send_sem.at[2], recv_sem=sm_sem.at[step % 2, d],
            device_id=peer(axis, hop), device_id_type=MESH,
        )

    def smt_copy(d):
        return pltpu.make_async_remote_copy(
            src_ref=smt_out.at[d], dst_ref=smt_in.at[d],
            send_sem=send_sem.at[3], recv_sem=smt_sem.at[d],
            device_id=peer("ta", (-1, 1)[d]), device_id_type=MESH,
        )

    def colour_hops(items, step, beside, take):
        vectors = unflat(items, 2)
        behinds = []
        for kind, mu in ((0, 1), (1, 2)):
            for i, v in enumerate(sh.pack(items, kind, True)):
                sm_out[step, 2 * kind, i] = v
            sm_copy(step, 2 * kind).start()
            behind = flat(link_times(link, mu, vectors, True))
            behinds.append(behind)
            for i, v in enumerate(sh.pack(behind, kind, False)):
                sm_out[step, 2 * kind + 1, i] = v
            sm_copy(step, 2 * kind + 1).start()
        beside()
        take(
            0,
            flat(link_times(link, 0, unflat(sh.along_x(items, True), 2), False)),
            sh.along_x(flat(link_times(link, 0, vectors, True)), False),
        )
        for kind, mu in ((0, 1), (1, 2)):
            sm_copy(step, 2 * kind).wait_recv()
            got = [sm_in[step, 2 * kind, i] for i in range(3)]
            ahead = unflat(sh.shift(items, got, kind, True), 2)
            ahead = flat(link_times(link, mu, ahead, False))
            sm_copy(step, 2 * kind + 1).wait_recv()
            got = [sm_in[step, 2 * kind + 1, i] for i in range(3)]
            take(mu, ahead, sh.shift(behinds[kind], got, kind, False))

    def smear_step(step, items, beside):
        total = [None] * 12

        def take(mu, ahead, behind):
            for i in range(12):
                part = ahead[i] + behind[i]
                total[i] = part if total[i] is None else total[i] + part

        colour_hops(list(items), step, beside, take)
        return tuple((v + 0.25 * t) * 0.5 for v, t in zip(items, total))

    def start_right(items):
        for i, v in enumerate(items):
            smt_out[0, i] = v
        smt_copy(0).start()
        for i, v in enumerate(flat(link_times(link, 3, unflat(items, 2), True))):
            smt_out[1, i] = v
        smt_copy(1).start()

    def finish_right(items, beside):
        def take(mu, ahead, behind):
            for i in range(12):
                hops[mu, i] = HOP * (behind[i] - ahead[i])
                part = HOP * (ahead[i] + behind[i])
                hops[4, i] = items[i] - part if mu == 0 else hops[4, i] - part

        colour_hops(items, NSMEAR, beside, take)
        smt_copy(0).wait_recv()
        got = unflat([smt_in[0, i] for i in range(12)], 2)
        ahead = flat(link_times(link, 3, got, False))
        smt_copy(1).wait_recv()
        take(3, ahead, [smt_in[1, i] for i in range(12)])
        zero = jnp.zeros((8, 128), jnp.float32)

        def pick(which, q, a):
            return hops[which, q * 3 + a], hops[which, 6 + q * 3 + a]

        def block(s2, s, q, a):
            if s2 == s:
                return pick(4, q, a)
            if s2 // 2 == s // 2:
                return (zero, zero)
            out = None
            for mu in range(4):
                for row in range(2):
                    column, coef = E_ROWS[mu][row]
                    if s2 < 2 and row == s2 and column == s - 2:
                        out = add_term(out or (zero, zero), coef, pick(mu, q, a))
                    if s2 >= 2 and column == s2 - 2 and row == s:
                        out = add_term(out or (zero, zero), complex(coef).conjugate(), pick(mu, q, a))
            return out

        for s2 in range(4):
            for a in range(3):
                column = [block(s2, s, 0, a) for s in range(4)]
                lone = [block(s2, s, 1, a) for s in range(4)]
                for part in range(2):
                    i = part * 12 + s2 * 3 + a
                    for s in range(4):
                        right[s, i] = column[s][part]
                    right[4, i] = jnp.where(sh.low, lone[0][part], lone[1][part])
                    right[5, i] = jnp.where(sh.low, lone[2][part], lone[3][part])

    def first_time(p, _):
        send_time(load_field(guess, p), 0, p, 1)
        return _

    def first_edges(p, _):
        send_edges(load_field(guess, p), 0, p, 1)
        return _

    row = lax.broadcasted_iota(jnp.int32, (8, 128), 0)
    hit = (row % 4 == sites_ref[1]) & (sh.lane == sites_ref[2] * LX + sites_ref[3])
    hit = hit & (sites_ref[0] == 0)
    one = jnp.where(hit, 1.0, 0.0).astype(jnp.float32)
    zero = jnp.zeros((8, 128), jnp.float32)
    upper, lower = jnp.where(sh.low, one, 0.0), jnp.where(sh.low, 0.0, one)
    items = tuple(flat([
        [(upper, zero), (lower, zero), (zero, zero)],
        [(zero, zero), (zero, zero), (one, zero)],
    ]))

    def second(p, _):
        out = receive_body(guess, 0, p, 1)
        for i, v in enumerate(out):
            field_a[p, i] = v
        send_time(unflat(out, 4), 1, p, -1)
        send_edges(unflat(out, 4), 1, p, -1)
        return _

    def third(p, _):
        out = [right[p, i] - v for i, v in enumerate(receive_body(field_a, 1, p, -1))]
        total = None
        for i, v in enumerate(out):
            search[p, i] = v
            total = v * v if total is None else total + v * v
        sums[p] = total
        send_time(unflat(out, 4), 2, p, 1)
        send_edges(unflat(out, 4), 2, p, 1)
        return _

    def run(body, first, end):
        lax.fori_loop(first, end, body, 0)

    def beside(step):
        if step == 0:
            run(first_time, 0, PAIRS)
            run(first_edges, 0, EDGE_CHUNK)
        if step == 1:
            run(first_edges, EDGE_CHUNK, PAIRS)
            interior(guess, 1)
        if 2 <= step < 2 + EARLY:
            run(second, step - 2, step - 1)
        if step == 2 + EARLY:
            interior(field_a, -1, 0, EARLY)
        if step == NSMEAR:
            run(second, EARLY, PAIRS)
            interior(field_a, -1, EARLY, PAIRS)

    for step in range(NSMEAR):
        items = smear_step(step, items, functools.partial(beside, step))
    items = list(items)
    start_right(items)
    finish_right(items, functools.partial(beside, NSMEAR))

    run(third, 0, PAIRS)
    interior(search, 1)

    def fourth(p, _):
        out = receive_body(search, 2, p, 1)
        total = None
        for i, v in enumerate(out):
            field_b[p, i] = v
            total = v * v if total is None else total + v * v
        sums[PAIRS + p] = total
        send_time(unflat(out, 4), 3, p, -1, held=True)
        send_edges(unflat(out, 4), 3, p, -1)
        return _

    run(fourth, 0, PAIRS)

    def normal_of(p, _):
        for i, v in enumerate(receive_body(field_b, 3, p, -1)):
            field_a[p, i] = v
        return _

    mine = jnp.zeros((8, 128), jnp.float32)
    for k in range(2 * PAIRS):
        mine = jnp.where(sh.lane == k, jnp.sum(sums[k], axis=1, keepdims=True), mine)
    slot = 0
    for stage, axis in enumerate(AXES):
        red_out[stage] = mine
        copies = []
        for k in range(1, n_of[axis]):
            copy = pltpu.make_async_remote_copy(
                src_ref=red_out.at[stage], dst_ref=red_in.at[slot],
                send_sem=send_sem.at[4], recv_sem=red_sem.at[slot],
                device_id=peer(axis, k), device_id_type=MESH,
            )
            copy.start()
            copies.append((copy, slot))
            slot += 1
        if stage == 0:
            interior(field_b, -1)
        if stage == 2:
            for d in range(2):
                time_copy(3, d, PAIRS - 1).start()
            run(normal_of, 0, PAIRS - 1)
        for copy, place in copies:
            copy.wait_recv()
            mine = mine + red_in[place]
    top = jnp.sum(mine[0:4], axis=0, keepdims=True)
    bottom = jnp.sum(mine[4:8], axis=0, keepdims=True)
    both = jnp.where(sh.low, top, bottom)
    curvature = pltpu.roll(both, 128 - PAIRS, 1)
    steps = both / jnp.where(sh.lane < PAIRS, curvature, 1.0)

    def last(p, _):
        length = jnp.sum(jnp.where(sh.lane == p, steps, 0.0), axis=1, keepdims=True)
        first, second_rhs = rhs_of(p)
        for i in range(24):
            s = search[p, i]
            res = s - length * field_a[p, i]
            sol = guess[p, i] + length * s
            res_ref[first, i] = res[0:4]
            res_ref[second_rhs, i] = res[4:8]
            sol_ref[first, i] = sol[0:4]
            sol_ref[second_rhs, i] = sol[4:8]
        return _

    run(last, 0, PAIRS - 1)
    run(normal_of, PAIRS - 1, PAIRS)
    run(last, PAIRS - 1, PAIRS)

    for k, (sent, landed) in enumerate((
        (edge_out, edge_in), (time_out, time_in), (sm_out, sm_in), (smt_out, smt_in), (red_in, red_in),
    )):
        pltpu.make_async_remote_copy(
            src_ref=sent, dst_ref=landed, send_sem=send_sem.at[k], recv_sem=red_sem.at[0],
            device_id=peer("ta", 1), device_id_type=MESH,
        ).wait_send()


def on_device(sizes, links, guess, source_sites):
    rows, lanes = guess.shape[-2:]
    f32 = jnp.float32
    copies = sum(n - 1 for n in sizes)
    tile = (8, lanes)
    vm = lambda *shape: pltpu.VMEM(shape + tile, f32)
    dma = lambda *shape: pltpu.SemaphoreType.DMA(shape)
    out = jax.ShapeDtypeStruct((12, 24, rows, lanes), f32)
    sol, res = pl.pallas_call(
        functools.partial(kernel, sizes),
        out_shape=(out, out),
        in_specs=[
            pl.BlockSpec(memory_space=pltpu.HBM),
            pl.BlockSpec(memory_space=pltpu.HBM),
            pl.BlockSpec(memory_space=pltpu.HBM),
        ],
        out_specs=(pl.BlockSpec(memory_space=pltpu.VMEM), pl.BlockSpec(memory_space=pltpu.VMEM)),
        scratch_shapes=[
            pltpu.SMEM((4,), jnp.int32), pltpu.VMEM((72, rows, lanes), f32), pltpu.VMEM((12, 24, rows, lanes), f32),
            vm(72), vm(PAIRS, 24), vm(PAIRS, 24), vm(PAIRS, 24), vm(PAIRS, 24), vm(PAIRS, 24),
            vm(PAIRS, 24), vm(2, PAIRS, 12),
            vm(4, 4, PAIRS, 3), vm(4, 4, PAIRS, 3), vm(4, 2, PAIRS, 12), vm(4, 2, PAIRS, 12),
            vm(NSMEAR + 1, 4, 3), vm(NSMEAR + 1, 4, 3), vm(2, 12), vm(2, 12),
            vm(3), vm(copies), vm(2 * PAIRS), vm(5, 12),
            dma(3), dma(2, 4, PAIRS // EDGE_CHUNK), dma(2, 2, PAIRS), dma(2, 4), dma(2), dma(copies), dma(5),
        ],
        compiler_params=pltpu.CompilerParams(
            collective_id=0, has_side_effects=True, vmem_limit_bytes=48 * 1024 * 1024
        ),
    )(*(
        pltpu.with_memory_space_constraint(x, pltpu.HBM)
        for x in (
            source_sites.reshape(4), links.reshape(72, rows, lanes), guess.reshape(12, 24, rows, lanes)
        )
    ))
    return sol.reshape(guess.shape), res.reshape(guess.shape)


def solution(mesh):
    sizes = tuple(mesh.shape[axis] for axis in AXES)
    fields = P(None, None, None, None, "ta", "xy", "gz")
    return jax.shard_map(
        functools.partial(on_device, sizes),
        mesh=mesh,
        in_specs=(fields, fields, P("ta", "xy", "gz", None)),
        out_specs=(fields, fields),
        check_vma=False,
    )
```

```python
import functools

import jax
import jax.numpy as jnp
from jax import lax
from jax.experimental import pallas as pl
from jax.experimental.pallas import tpu as pltpu
from jax.sharding import PartitionSpec as P

LX = 32
NSMEAR = 8
HOP = 0.12
PAIRS = 6
EDGE_CHUNK = 3
TIME_CHUNK = 1
MESH = pl.DeviceIdType.MESH
AXES = ("xy", "gz", "ta")

E_ROWS = (
    ((1, -1j), (0, -1j)),
    ((1, -1), (0, 1)),
    ((0, -1j), (1, 1j)),
    ((0, 1), (1, 1)),
)


def times(coef, z):
    re, im = z
    if coef == 1:
        return (1, re), (1, im)
    if coef == -1:
        return (-1, re), (-1, im)
    if coef == 1j:
        return (-1, im), (1, re)
    return (1, im), (-1, re)


def add_term(z, coef, other):
    out = []
    for base, (sign, term) in zip(z, times(coef, other)):
        out.append(base + term if sign > 0 else base - term)
    return tuple(out)


def project(f, mu, parity):
    half = []
    for row in range(2):
        column, coef = E_ROWS[mu][row]
        half.append([add_term(f[row][a], parity * coef, f[2 + column][a]) for a in range(3)])
    return half


def lift_add(total, h, mu, parity):
    for row in range(2):
        column, coef = E_ROWS[mu][row]
        for a in range(3):
            total[row][a] = add_term(total[row][a], 1, h[row][a])
            low = parity * complex(coef).conjugate()
            total[2 + column][a] = add_term(total[2 + column][a], low, h[row][a])


def link_times(link, mu, vectors, adjoint):
    def entry(a, b):
        if adjoint:
            a, b = b, a
        base = mu * 18 + a * 3 + b
        return link[base], link[base + 9]

    out = [[None] * 3 for _ in vectors]
    for a in range(3):
        totals = [None] * len(vectors)
        for b in range(3):
            ur, ui = entry(a, b)
            for k, vec in enumerate(vectors):
                re, im = vec[b]
                if adjoint:
                    tr, ti = ur * re + ui * im, ur * im - ui * re
                else:
                    tr, ti = ur * re - ui * im, ur * im + ui * re
                old = totals[k]
                totals[k] = (tr, ti) if old is None else (old[0] + tr, old[1] + ti)
        for k in range(len(vectors)):
            out[k][a] = totals[k]
    return out


def flat(vectors):
    return [vec[a][part] for part in range(2) for vec in vectors for a in range(3)]


def unflat(items, count):
    return [
        [(items[k * 3 + a], items[3 * count + k * 3 + a]) for a in range(3)] for k in range(count)
    ]


class Shifts:
    def __init__(self):
        row = lax.broadcasted_iota(jnp.int32, (8, 128), 0)
        lane = lax.broadcasted_iota(jnp.int32, (8, 128), 1)
        self.low = row < 4
        self.row = row
        self.lane = lane
        self.place = ([row % 4 == k for k in range(4)], [lane // LX == k for k in range(4)])
        self.x_first = lane % LX == 0
        self.x_last = lane % LX == LX - 1
        self.unit = ((0, 1, 8), (1, LX, 128))

    def roll(self, v, kind, steps):
        axis, unit, size = self.unit[kind]
        amount = (steps * unit) % size
        return v if amount == 0 else pltpu.roll(v, amount, axis)

    def pack(self, items, kind, ahead):
        packed = []
        for g in range(0, len(items), 4):
            out = None
            for k in range(4):
                v = self.roll(items[g + k], kind, k if ahead else k - 3)
                out = v if out is None else jnp.where(self.place[kind][k], v, out)
            packed.append(out)
        return packed

    def shift(self, items, packed, kind, ahead):
        outs = []
        for i, v in enumerate(items):
            got = packed[i // 4]
            k = i % 4
            if ahead:
                moved = self.roll(v, kind, -1)
                outs.append(jnp.where(self.place[kind][3], self.roll(got, kind, 3 - k), moved))
            else:
                moved = self.roll(v, kind, 1)
                outs.append(jnp.where(self.place[kind][0], self.roll(got, kind, -k), moved))
        return outs

    def along_x(self, items, ahead):
        outs = []
        for v in items:
            if ahead:
                a, b = pltpu.roll(v, 127, 1), pltpu.roll(v, LX - 1, 1)
                outs.append(jnp.where(self.x_last, b, a))
            else:
                a, b = pltpu.roll(v, 1, 1), pltpu.roll(v, 129 - LX, 1)
                outs.append(jnp.where(self.x_first, b, a))
        return outs


def kernel(
    sizes, sites_hbm, links_hbm, guess_hbm, search_ref, normal_ref, length_ref,
    sites_ref, links_ref, guess_ref, blocks, wide, smear, carry,
    link, guess, field_a, field_b, search, acc, right, carried,
    edge_out, edge_in, time_out, time_in, smt_out, smt_in,
    red_out, red_in, sums, hops,
    load_sem, edge_sem, time_sem, block_sem, smt_sem, red_sem, send_sem,
):
    n_of = dict(zip(AXES, sizes))
    me = {axis: lax.axis_index(axis) for axis in AXES}
    n_gz = n_of["gz"]
    reach = min(n_of["xy"], 8)
    own = 0 if reach == n_of["xy"] else reach // 2
    groups = reach // 2

    loads = [
        pltpu.make_async_copy(src, dst, load_sem.at[k])
        for k, (src, dst) in enumerate((
            (links_hbm, links_ref), (sites_hbm, sites_ref), (guess_hbm, guess_ref),
            (links_hbm.at[pl.ds(0, 54)], blocks.at[own * n_gz + me["gz"], pl.ds(1, 54)]),
        ))
    ]
    for k in (3, 1, 0, 2):
        loads[k].start()

    def peer(axis, step):
        return {axis: lax.rem(me[axis] + step + n_of[axis], n_of[axis])}

    def across(xy, gz):
        return {
            "xy": lax.rem(me["xy"] + xy + n_of["xy"], n_of["xy"]),
            "gz": lax.rem(me["gz"] + gz + n_gz, n_gz),
        }

    shifts = sorted({(slot - own) % n_of["xy"] for slot in range(reach)} | {(own - slot) % n_of["xy"] for slot in range(reach)})
    greeted = [across(y, z) for y in shifts for z in range(n_gz) if (y, z) != (0, 0)]
    greeted += [peer("xy", y) for y in range(1, n_of["xy"]) if y not in shifts]
    greeted += [peer("ta", t) for t in range(1, n_of["ta"])]
    barrier = pltpu.get_barrier_semaphore()
    for device in greeted:
        pl.semaphore_signal(barrier, inc=1, device_id=device, device_id_type=MESH)

    sh = Shifts()

    row = lax.broadcasted_iota(jnp.int32, (4, 128), 0)
    lane = lax.broadcasted_iota(jnp.int32, (4, 128), 1)
    loads[3].wait()
    loads[1].wait()
    hit = (row == sites_ref[1]) & (lane == sites_ref[2] * LX + sites_ref[3])
    hit = hit & (sites_ref[0] == 0)
    blocks[own * n_gz + me["gz"], 0] = jnp.where(hit, 1.0, 0.0).astype(jnp.float32)

    loads[0].wait()
    sign = jnp.where(me["ta"] == n_of["ta"] - 1, -1.0, 1.0).astype(jnp.float32)
    for i in range(72):
        v = links_ref[i]
        if i >= 54:
            v = v * sign
        link[i, 0:4, :] = v
        link[i, 4:8, :] = v

    def rhs_of(p):
        first = jnp.where(p < 4, 3 * p, 6 * p - 22)
        second = jnp.where(p < 4, 3 * p + 1, 6 * p - 19)
        return first, second

    def load_guess(p, _):
        first, second = rhs_of(p)
        for i in range(24):
            guess[p, i, 0:4, :] = guess_ref[first, i]
            guess[p, i, 4:8, :] = guess_ref[second, i]
        return _

    loads[2].wait()
    lax.fori_loop(0, PAIRS, load_guess, 0)
    pl.semaphore_wait(barrier, len(greeted))

    def part_of(p, chunk):
        return pl.ds(p, chunk)

    def start_last(make, w, d, p, chunk):
        if chunk == 1:
            make(w, d, p).start()
        else:
            @pl.when(lax.rem(p, chunk) == chunk - 1)
            def _():
                make(w, d, p - (chunk - 1)).start()

    def await_first(make, w, p, chunk, dirs):
        def wait():
            for d in dirs:
                make(w, d, p).wait_recv()
        if chunk == 1:
            wait()
        else:
            pl.when(lax.rem(p, chunk) == 0)(wait)

    def edge_copy(w, d, p):
        axis, step = (("xy", -1), ("xy", 1), ("gz", -1), ("gz", 1))[d]
        return pltpu.make_async_remote_copy(
            src_ref=edge_out.at[w, d, part_of(p, EDGE_CHUNK)], dst_ref=edge_in.at[w, d, part_of(p, EDGE_CHUNK)],
            send_sem=send_sem.at[0], recv_sem=edge_sem.at[lax.rem(w, 2), d, p // EDGE_CHUNK],
            device_id=peer(axis, step), device_id_type=MESH,
        )

    def time_copy(w, d, p):
        return pltpu.make_async_remote_copy(
            src_ref=time_out.at[w, d, part_of(p, TIME_CHUNK)], dst_ref=time_in.at[w, d, part_of(p, TIME_CHUNK)],
            send_sem=send_sem.at[1], recv_sem=time_sem.at[lax.rem(w, 2), d, p],
            device_id=peer("ta", (-1, 1)[d]), device_id_type=MESH,
        )

    def load_field(ref, p):
        return unflat([ref[p, i] for i in range(24)], 4)

    def send_time(f, w, p, par, held=False):
        def start(d):
            if held:
                pl.when(p < PAIRS - 1)(lambda: time_copy(w, d, p).start())
            else:
                time_copy(w, d, p).start()

        for i, v in enumerate(flat(project(f, 3, -par))):
            time_out[w, 0, p, i] = v
        start(0)
        for i, v in enumerate(flat(link_times(link, 3, project(f, 3, par), True))):
            time_out[w, 1, p, i] = v
        start(1)

    def send_edges(f, w, p, par):
        for kind, mu in ((0, 1), (1, 2)):
            for i, v in enumerate(sh.pack(flat(project(f, mu, -par)), kind, True)):
                edge_out[w, 2 * kind, p, i] = v
            start_last(edge_copy, w, 2 * kind, p, EDGE_CHUNK)
            behind = flat(link_times(link, mu, project(f, mu, par), True))
            for i, v in enumerate(behind):
                carried[kind, p, i] = v
            for i, v in enumerate(sh.pack(behind, kind, False)):
                edge_out[w, 2 * kind + 1, p, i] = v
            start_last(edge_copy, w, 2 * kind + 1, p, EDGE_CHUNK)

    def interior(src, par, first=0, end=PAIRS):
        def body(p, _):
            f = load_field(src, p)
            zero = jnp.zeros((8, 128), jnp.float32)
            total = [[(zero, zero)] * 3 for _ in range(4)]
            ahead = unflat(sh.along_x(flat(project(f, 0, -par)), True), 2)
            lift_add(total, link_times(link, 0, ahead, False), 0, -par)
            behind = flat(link_times(link, 0, project(f, 0, par), True))
            lift_add(total, unflat(sh.along_x(behind, False), 2), 0, par)
            for i, v in enumerate(flat(total)):
                acc[p, i] = v
            return _
        lax.fori_loop(first, end, body, 0)

    def receive_body(src, w, p, par):
        await_first(edge_copy, w, p, EDGE_CHUNK, range(4))
        await_first(time_copy, w, p, TIME_CHUNK, range(2))
        f = load_field(src, p)
        total = load_field(acc, p)
        for kind, mu in ((0, 1), (1, 2)):
            got = [edge_in[w, 2 * kind, p, i] for i in range(3)]
            ahead = unflat(sh.shift(flat(project(f, mu, -par)), got, kind, True), 2)
            lift_add(total, link_times(link, mu, ahead, False), mu, -par)
            got = [edge_in[w, 2 * kind + 1, p, i] for i in range(3)]
            local = [carried[kind, p, i] for i in range(12)]
            lift_add(total, unflat(sh.shift(local, got, kind, False), 2), mu, par)
        ahead = unflat([time_in[w, 0, p, i] for i in range(12)], 2)
        lift_add(total, link_times(link, 3, ahead, False), 3, -par)
        lift_add(total, unflat([time_in[w, 1, p, i] for i in range(12)], 2), 3, par)
        return [a - HOP * b for a, b in zip(flat(f), flat(total))]

    def block_copy(slot, gz, device, to):
        return pltpu.make_async_remote_copy(
            src_ref=blocks.at[slot * n_gz + gz], dst_ref=blocks.at[to * n_gz + gz],
            send_sem=send_sem.at[2], recv_sem=block_sem.at[to * n_gz + gz],
            device_id=device, device_id_type=MESH,
        )

    mate = 1 - 2 * lax.rem(me["gz"], 2)
    direct = [(slot, z) for z in range(0, n_gz, 2) for slot in range(reach) if (slot, z) != (own, 0)]

    def send_blocks():
        block_copy(own, me["gz"], across(0, mate), own).start()
        for slot, z in direct:
            block_copy(own, me["gz"], across(own - slot, z), slot).start()

    def pass_blocks():
        for slot, z in direct:
            copy = block_copy(slot, lax.rem(me["gz"] - z + n_gz, n_gz), across(0, mate), slot)
            copy.wait_recv()
            copy.start()

    def await_blocks():
        for z in range(0, n_gz, 2):
            for slot in range(reach):
                block_copy(slot, lax.rem(me["gz"] + mate - z + 2 * n_gz, n_gz), across(0, mate), slot).wait_recv()

    def smt_copy(d):
        return pltpu.make_async_remote_copy(
            src_ref=smt_out.at[d], dst_ref=smt_in.at[d],
            send_sem=send_sem.at[3], recv_sem=smt_sem.at[d],
            device_id=peer("ta", (-1, 1)[d]), device_id_type=MESH,
        )

    def widen(z, _):
        zero = jnp.zeros((8, 128), jnp.float32)
        for g in range(groups):
            for i in range(55):
                wide[g, z, i, 0:4] = blocks[2 * g * n_gz + z, i]
                wide[g, z, i, 4:8] = blocks[(2 * g + 1) * n_gz + z, i]
            for c in range(3):
                for i in range(6):
                    smear[0, g, z, c * 6 + i] = wide[g, z, 0] if i == c else zero
            carry_hops(0, g, z)
        return _

    def links_of(g, z):
        return wide.at[g, z, pl.ds(1, 54)]

    def colour(ref, now, g, z, c):
        return [ref[now, g, z, c * 6 + i] for i in range(6)]

    def carry_hops(now, g, z):
        for c in range(3):
            vector = unflat(colour(smear, now, g, z, c), 1)
            for mu in (2,) if groups == 1 else (2, 1):
                for i, v in enumerate(flat(link_times(links_of(g, z), mu, vector, True))):
                    carry[2 - mu, now, g, z, c * 6 + i] = v

    def beyond(items, others, kind, ahead):
        outs = []
        for v, other in zip(items, others):
            step = -1 if ahead else 1
            inner = (sh.row if kind == 0 else sh.lane // LX)
            last = inner == ((7, 3)[kind] if ahead else 0)
            moved = sh.roll(v, kind, step)
            outs.append(moved if other is None else jnp.where(last, sh.roll(other, kind, step), moved))
        return outs

    def colour_hops(now, g, z, c):
        link_at = links_of(g, z)
        items = colour(smear, now, g, z, c)
        vector = unflat(items, 1)
        out = [(
            flat(link_times(link_at, 0, unflat(sh.along_x(items, True), 1), False)),
            sh.along_x(flat(link_times(link_at, 0, vector, True)), False),
        )]
        if groups == 1:
            later, behind, before = [None] * 6, flat(link_times(link_at, 1, vector, True)), [None] * 6
        else:
            later = colour(smear, now, (g + 1) % groups, z, c)
            behind = colour(carry.at[1], now, g, z, c)
            before = colour(carry.at[1], now, (g - 1) % groups, z, c)
        out.append((
            flat(link_times(link_at, 1, unflat(beyond(items, later, 0, True), 1), False)),
            beyond(behind, before, 0, False),
        ))
        later = colour(smear, now, g, lax.rem(z + 1, n_gz), c)
        behind = colour(carry.at[0], now, g, z, c)
        before = colour(carry.at[0], now, g, lax.rem(z + n_gz - 1, n_gz), c)
        out.append((
            flat(link_times(link_at, 2, unflat(beyond(items, later, 1, True), 1), False)),
            beyond(behind, before, 1, False),
        ))
        return items, out

    def smear_steps(first, end):
        for step in range(first, end):
            now, then = step % 2, (step + 1) % 2
            deep = min(-(-(NSMEAR - step) // (128 // LX)), n_gz // 2)

            def body(k, _):
                z = lax.rem(me["gz"] - deep + k + n_gz, n_gz)
                for g in range(groups):
                    for c in range(3):
                        items, parts = colour_hops(now, g, z, c)
                        for i, v in enumerate(items):
                            total = None
                            for ahead, behind in parts:
                                part = ahead[i] + behind[i]
                                total = part if total is None else total + part
                            smear[then, g, z, c * 6 + i] = (v + 0.25 * total) * 0.5
                    carry_hops(then, g, z)
                return _

            lax.fori_loop(0, min(2 * deep + 1, n_gz), body, 0)

    def paired(colours):
        out = []
        for part in range(2):
            for q in range(2):
                for a in range(3):
                    i = part * 3 + a
                    up, down = colours[2 * q][i], colours[1 + q][i]
                    out.append(jnp.where(sh.low, up, pltpu.roll(down, 4, 0)))
        return out

    def start_right(items):
        for i, v in enumerate(items):
            smt_out[0, i] = v
        smt_copy(0).start()
        for i, v in enumerate(flat(link_times(link, 3, unflat(items, 2), True))):
            smt_out[1, i] = v
        smt_copy(1).start()

    def local_right(items):
        done = [colour_hops(NSMEAR % 2, own // 2, me["gz"], c)[1] for c in range(3)]
        for mu in range(3):
            take(mu, items, *(paired([parts[mu][side] for parts in done]) for side in range(2)))

    def take(mu, items, ahead, behind):
        for i in range(12):
            hops[mu, i] = HOP * (behind[i] - ahead[i])
            part = HOP * (ahead[i] + behind[i])
            hops[4, i] = items[i] - part if mu == 0 else hops[4, i] - part

    def finish_right():
        smt_copy(0).wait_recv()
        got = unflat([smt_in[0, i] for i in range(12)], 2)
        ahead = flat(link_times(link, 3, got, False))
        smt_copy(1).wait_recv()
        take(3, None, ahead, [smt_in[1, i] for i in range(12)])
        zero = jnp.zeros((8, 128), jnp.float32)

        def pick(which, q, a):
            return hops[which, q * 3 + a], hops[which, 6 + q * 3 + a]

        def block(s2, s, q, a):
            if s2 == s:
                return pick(4, q, a)
            if s2 // 2 == s // 2:
                return (zero, zero)
            out = None
            for mu in range(4):
                for row in range(2):
                    column, coef = E_ROWS[mu][row]
                    if s2 < 2 and row == s2 and column == s - 2:
                        out = add_term(out or (zero, zero), coef, pick(mu, q, a))
                    if s2 >= 2 and column == s2 - 2 and row == s:
                        out = add_term(out or (zero, zero), complex(coef).conjugate(), pick(mu, q, a))
            return out

        for s2 in range(4):
            for a in range(3):
                column = [block(s2, s, 0, a) for s in range(4)]
                lone = [block(s2, s, 1, a) for s in range(4)]
                for part in range(2):
                    i = part * 12 + s2 * 3 + a
                    for s in range(4):
                        right[s, i] = column[s][part]
                    right[4, i] = jnp.where(sh.low, lone[0][part], lone[1][part])
                    right[5, i] = jnp.where(sh.low, lone[2][part], lone[3][part])

    def first_time(p, _):
        send_time(load_field(guess, p), 0, p, 1)
        return _

    def first_edges(p, _):
        send_edges(load_field(guess, p), 0, p, 1)
        return _

    def give(ref, p, out):
        first, second_rhs = rhs_of(p)
        for i, v in enumerate(out):
            ref[first, i] = v[0:4]
            ref[second_rhs, i] = v[4:8]

    def second(p, _):
        out = receive_body(guess, 0, p, 1)
        for i, v in enumerate(out):
            field_a[p, i] = v
        send_time(unflat(out, 4), 1, p, -1)
        send_edges(unflat(out, 4), 1, p, -1)
        return _

    def third(p, _):
        out = [right[p, i] - v for i, v in enumerate(receive_body(field_a, 1, p, -1))]
        total = None
        for i, v in enumerate(out):
            search[p, i] = v
            total = v * v if total is None else total + v * v
        sums[p] = total
        give(search_ref, p, out)
        send_time(unflat(out, 4), 2, p, 1)
        send_edges(unflat(out, 4), 2, p, 1)
        return _

    def run(body, first, end):
        lax.fori_loop(first, end, body, 0)

    send_blocks()
    run(first_time, 0, PAIRS)
    run(first_edges, 0, PAIRS)
    interior(guess, 1)
    pass_blocks()
    run(second, 0, 2)
    await_blocks()
    lax.fori_loop(0, n_gz, widen, 0)
    smear_steps(0, 3)
    run(second, 2, 3)
    smear_steps(3, NSMEAR)
    items = paired([colour(smear, NSMEAR % 2, own // 2, me["gz"], c) for c in range(3)])
    start_right(items)
    run(second, 3, PAIRS)
    local_right(items)
    interior(field_a, -1)
    finish_right()

    run(third, 0, PAIRS)
    interior(search, 1)

    def fourth(p, _):
        out = receive_body(search, 2, p, 1)
        total = None
        for i, v in enumerate(out):
            field_b[p, i] = v
            total = v * v if total is None else total + v * v
        sums[PAIRS + p] = total
        send_time(unflat(out, 4), 3, p, -1, held=True)
        send_edges(unflat(out, 4), 3, p, -1)
        return _

    run(fourth, 0, PAIRS)

    def normal_of(p, _):
        give(normal_ref, p, receive_body(field_b, 3, p, -1))
        return _

    mine = jnp.zeros((8, 128), jnp.float32)
    for k in range(2 * PAIRS):
        mine = jnp.where(sh.lane == k, jnp.sum(sums[k], axis=1, keepdims=True), mine)
    slot = 0
    for stage, axis in enumerate(AXES):
        red_out[stage] = mine
        copies = []
        for k in range(1, n_of[axis]):
            copy = pltpu.make_async_remote_copy(
                src_ref=red_out.at[stage], dst_ref=red_in.at[slot],
                send_sem=send_sem.at[4], recv_sem=red_sem.at[slot],
                device_id=peer(axis, k), device_id_type=MESH,
            )
            copy.start()
            copies.append((copy, slot))
            slot += 1
        if stage == 0:
            interior(field_b, -1)
        if stage == 2:
            for d in range(2):
                time_copy(3, d, PAIRS - 1).start()
            run(normal_of, 0, PAIRS - 1)
        for copy, place in copies:
            copy.wait_recv()
            mine = mine + red_in[place]
    top = jnp.sum(mine[0:4], axis=0, keepdims=True)
    bottom = jnp.sum(mine[4:8], axis=0, keepdims=True)
    both = jnp.where(sh.low, top, bottom)
    curvature = pltpu.roll(both, 128 - PAIRS, 1)
    steps = both / jnp.where(sh.lane < PAIRS, curvature, 1.0)

    run(normal_of, PAIRS - 1, PAIRS)
    for p in range(PAIRS):
        length = jnp.sum(jnp.where(sh.lane == p, steps, 0.0), axis=1, keepdims=True)
        first, second_rhs = (3 * p, 3 * p + 1) if p < 4 else (6 * p - 22, 6 * p - 19)
        length_ref[first : first + 1] = jnp.broadcast_to(length[0:1], (1, 128))
        length_ref[second_rhs : second_rhs + 1] = jnp.broadcast_to(length[4:5], (1, 128))

    passed = blocks.at[pl.ds(0, reach * n_gz - 1)]
    for k, (sent, landed) in enumerate((
        (edge_out, edge_in), (time_out, time_in), (passed, passed), (smt_out, smt_in), (red_in, red_in),
    )):
        pltpu.make_async_remote_copy(
            src_ref=sent, dst_ref=landed, send_sem=send_sem.at[k], recv_sem=red_sem.at[0],
            device_id=peer("ta", 1), device_id_type=MESH,
        ).wait_send()


def on_device(sizes, links, guess, source_sites):
    rows, lanes = guess.shape[-2:]
    f32 = jnp.float32
    copies = sum(n - 1 for n in sizes)
    n_gz = sizes[AXES.index("gz")]
    reach = min(sizes[0], 8)
    groups = reach // 2
    tile = (8, lanes)
    vm = lambda *shape: pltpu.VMEM(shape + tile, f32)
    dma = lambda *shape: pltpu.SemaphoreType.DMA(shape)
    out = jax.ShapeDtypeStruct((12, 24, rows, lanes), f32)
    search, normal, length = pl.pallas_call(
        functools.partial(kernel, sizes),
        out_shape=(out, out, jax.ShapeDtypeStruct((12, lanes), f32)),
        in_specs=[
            pl.BlockSpec(memory_space=pltpu.HBM),
            pl.BlockSpec(memory_space=pltpu.HBM),
            pl.BlockSpec(memory_space=pltpu.HBM),
        ],
        out_specs=(pl.BlockSpec(memory_space=pltpu.VMEM),) * 3,
        scratch_shapes=[
            pltpu.SMEM((4,), jnp.int32), pltpu.VMEM((72, rows, lanes), f32), pltpu.VMEM((12, 24, rows, lanes), f32),
            pltpu.VMEM((reach * n_gz, 55, rows, lanes), f32), vm(groups, n_gz, 55),
            vm(2, groups, n_gz, 18), vm(min(groups, 2), 2, groups, n_gz, 18),
            vm(72), vm(PAIRS, 24), vm(PAIRS, 24), vm(PAIRS, 24), vm(PAIRS, 24), vm(PAIRS, 24),
            vm(PAIRS, 24), vm(2, PAIRS, 12),
            vm(4, 4, PAIRS, 3), vm(4, 4, PAIRS, 3), vm(4, 2, PAIRS, 12), vm(4, 2, PAIRS, 12),
            vm(2, 12), vm(2, 12),
            vm(3), vm(copies), vm(2 * PAIRS), vm(5, 12),
            dma(4), dma(2, 4, PAIRS // EDGE_CHUNK), dma(2, 2, PAIRS), dma(reach * n_gz), dma(2), dma(copies), dma(5),
        ],
        compiler_params=pltpu.CompilerParams(
            collective_id=0, has_side_effects=True, vmem_limit_bytes=48 * 1024 * 1024
        ),
    )(*(
        pltpu.with_memory_space_constraint(x, pltpu.HBM)
        for x in (
            source_sites.reshape(4), links.reshape(72, rows, lanes), guess.reshape(12, 24, rows, lanes)
        )
    ))
    length = length[:, None, None]
    sol = guess.reshape(search.shape) + length * search
    res = search - length * normal
    return sol.reshape(guess.shape), res.reshape(guess.shape)


def solution(mesh):
    sizes = tuple(mesh.shape[axis] for axis in AXES)
    fields = P(None, None, None, None, "ta", "xy", "gz")
    return jax.shard_map(
        functools.partial(on_device, sizes),
        mesh=mesh,
        in_specs=(fields, fields, P("ta", "xy", "gz", None)),
        out_specs=(fields, fields),
        check_vma=False,
    )
```

```python
import functools

import jax
import jax.numpy as jnp
from jax import lax
from jax.experimental import pallas as pl
from jax.experimental.pallas import tpu as pltpu
from jax.sharding import PartitionSpec as P

LX = 32
NSMEAR = 8
HOP = 0.12
PAIRS = 6
EDGE_CHUNK = 3
TIME_CHUNK = 1
MESH = pl.DeviceIdType.MESH
AXES = ("xy", "gz", "ta")

E_ROWS = (
    ((1, -1j), (0, -1j)),
    ((1, -1), (0, 1)),
    ((0, -1j), (1, 1j)),
    ((0, 1), (1, 1)),
)


def times(coef, z):
    re, im = z
    if coef == 1:
        return (1, re), (1, im)
    if coef == -1:
        return (-1, re), (-1, im)
    if coef == 1j:
        return (-1, im), (1, re)
    return (1, im), (-1, re)


def add_term(z, coef, other):
    out = []
    for base, (sign, term) in zip(z, times(coef, other)):
        out.append(base + term if sign > 0 else base - term)
    return tuple(out)


def project(f, mu, parity):
    half = []
    for row in range(2):
        column, coef = E_ROWS[mu][row]
        half.append([add_term(f[row][a], parity * coef, f[2 + column][a]) for a in range(3)])
    return half


def lift_add(total, h, mu, parity):
    for row in range(2):
        column, coef = E_ROWS[mu][row]
        for a in range(3):
            total[row][a] = add_term(total[row][a], 1, h[row][a])
            low = parity * complex(coef).conjugate()
            total[2 + column][a] = add_term(total[2 + column][a], low, h[row][a])


def link_times(link, mu, vectors, adjoint):
    def entry(a, b):
        if adjoint:
            a, b = b, a
        base = mu * 18 + a * 3 + b
        return link[base], link[base + 9]

    out = [[None] * 3 for _ in vectors]
    for a in range(3):
        totals = [None] * len(vectors)
        for b in range(3):
            ur, ui = entry(a, b)
            for k, vec in enumerate(vectors):
                re, im = vec[b]
                if adjoint:
                    tr, ti = ur * re + ui * im, ur * im - ui * re
                else:
                    tr, ti = ur * re - ui * im, ur * im + ui * re
                old = totals[k]
                totals[k] = (tr, ti) if old is None else (old[0] + tr, old[1] + ti)
        for k in range(len(vectors)):
            out[k][a] = totals[k]
    return out


def flat(vectors):
    return [vec[a][part] for part in range(2) for vec in vectors for a in range(3)]


def unflat(items, count):
    return [
        [(items[k * 3 + a], items[3 * count + k * 3 + a]) for a in range(3)] for k in range(count)
    ]


class Shifts:
    def __init__(self):
        row = lax.broadcasted_iota(jnp.int32, (8, 128), 0)
        lane = lax.broadcasted_iota(jnp.int32, (8, 128), 1)
        self.low = row < 4
        self.row = row
        self.lane = lane
        self.place = ([row % 4 == k for k in range(4)], [lane // LX == k for k in range(4)])
        self.x_first = lane % LX == 0
        self.x_last = lane % LX == LX - 1
        self.unit = ((0, 1, 8), (1, LX, 128))

    def roll(self, v, kind, steps):
        axis, unit, size = self.unit[kind]
        amount = (steps * unit) % size
        return v if amount == 0 else pltpu.roll(v, amount, axis)

    def pack(self, items, kind, ahead):
        packed = []
        for g in range(0, len(items), 4):
            out = None
            for k in range(4):
                v = self.roll(items[g + k], kind, k if ahead else k - 3)
                out = v if out is None else jnp.where(self.place[kind][k], v, out)
            packed.append(out)
        return packed

    def shift(self, items, packed, kind, ahead):
        outs = []
        for i, v in enumerate(items):
            got = packed[i // 4]
            k = i % 4
            if ahead:
                moved = self.roll(v, kind, -1)
                outs.append(jnp.where(self.place[kind][3], self.roll(got, kind, 3 - k), moved))
            else:
                moved = self.roll(v, kind, 1)
                outs.append(jnp.where(self.place[kind][0], self.roll(got, kind, -k), moved))
        return outs

    def along_x(self, items, ahead):
        outs = []
        for v in items:
            if ahead:
                a, b = pltpu.roll(v, 127, 1), pltpu.roll(v, LX - 1, 1)
                outs.append(jnp.where(self.x_last, b, a))
            else:
                a, b = pltpu.roll(v, 1, 1), pltpu.roll(v, 129 - LX, 1)
                outs.append(jnp.where(self.x_first, b, a))
        return outs


def kernel(
    sizes, sites_hbm, links_hbm, guess_hbm, search_ref, normal_ref, length_ref,
    sites_ref, links_ref, guess_ref, blocks, wide, smear, carry,
    link, guess, field_a, field_b, search, acc, right, carried,
    edge_out, edge_in, time_out, time_in, smt_out, smt_in,
    red_out, red_in, sums, hops, sources,
    load_sem, edge_sem, time_sem, block_sem, smt_sem, red_sem, send_sem,
):
    n_of = dict(zip(AXES, sizes))
    me = {axis: lax.axis_index(axis) for axis in AXES}
    n_gz = n_of["gz"]
    reach = min(n_of["xy"], 8)
    own = 0 if reach == n_of["xy"] else reach // 2
    groups = reach // 2

    loads = [
        pltpu.make_async_copy(src, dst, load_sem.at[k])
        for k, (src, dst) in enumerate((
            (links_hbm, links_ref), (sites_hbm, sites_ref), (guess_hbm, guess_ref),
            (links_hbm.at[pl.ds(0, 54)], blocks.at[own * n_gz + me["gz"], pl.ds(1, 54)]),
        ))
    ]
    for k in (3, 1, 0, 2):
        loads[k].start()

    def peer(axis, step):
        return {axis: lax.rem(me[axis] + step + n_of[axis], n_of[axis])}

    def across(xy, gz):
        return {
            "xy": lax.rem(me["xy"] + xy + n_of["xy"], n_of["xy"]),
            "gz": lax.rem(me["gz"] + gz + n_gz, n_gz),
        }

    shifts = sorted({(slot - own) % n_of["xy"] for slot in range(reach)} | {(own - slot) % n_of["xy"] for slot in range(reach)})
    greeted = [across(y, z) for y in shifts for z in range(n_gz) if (y, z) != (0, 0)]
    greeted += [peer("xy", y) for y in range(1, n_of["xy"]) if y not in shifts]
    greeted += [peer("ta", t) for t in range(1, n_of["ta"])]
    barrier = pltpu.get_barrier_semaphore()
    for device in greeted:
        pl.semaphore_signal(barrier, inc=1, device_id=device, device_id_type=MESH)

    sh = Shifts()

    row = lax.broadcasted_iota(jnp.int32, (4, 128), 0)
    lane = lax.broadcasted_iota(jnp.int32, (4, 128), 1)
    loads[3].wait()
    loads[1].wait()
    hit = (row == sites_ref[1]) & (lane == sites_ref[2] * LX + sites_ref[3])
    hit = hit & (sites_ref[0] == 0)
    blocks[own * n_gz + me["gz"], 0] = jnp.where(hit, 1.0, 0.0).astype(jnp.float32)

    loads[0].wait()
    sign = jnp.where(me["ta"] == n_of["ta"] - 1, -1.0, 1.0).astype(jnp.float32)

    def double_links(first, end):
        for i in range(first, end):
            v = links_ref[i]
            if i >= 54:
                v = v * sign
            link[i, 0:4, :] = v
            link[i, 4:8, :] = v

    double_links(54, 72)

    def rhs_of(p):
        first = 6 * lax.rem(p, 2) + p // 2
        return first, first + 3

    def load_guess(p, _):
        first, second = rhs_of(p)
        for i in range(24):
            guess[p, i, 0:4, :] = guess_ref[first, i]
            guess[p, i, 4:8, :] = guess_ref[second, i]
        return _

    loads[2].wait()
    pl.semaphore_wait(barrier, len(greeted))

    def part_of(p, chunk):
        return pl.ds(p, chunk)

    def start_last(make, w, d, p, chunk):
        if chunk == 1:
            make(w, d, p).start()
        else:
            @pl.when(lax.rem(p, chunk) == chunk - 1)
            def _():
                make(w, d, p - (chunk - 1)).start()

    def await_first(make, w, p, chunk, dirs):
        def wait():
            for d in dirs:
                make(w, d, p).wait_recv()
        if chunk == 1:
            wait()
        else:
            pl.when(lax.rem(p, chunk) == 0)(wait)

    def edge_copy(w, d, p):
        axis, step = (("xy", -1), ("xy", 1), ("gz", -1), ("gz", 1))[d]
        return pltpu.make_async_remote_copy(
            src_ref=edge_out.at[w, d, part_of(p, EDGE_CHUNK)], dst_ref=edge_in.at[w, d, part_of(p, EDGE_CHUNK)],
            send_sem=send_sem.at[0], recv_sem=edge_sem.at[lax.rem(w, 2), d, p // EDGE_CHUNK],
            device_id=peer(axis, step), device_id_type=MESH,
        )

    def time_copy(w, d, p):
        return pltpu.make_async_remote_copy(
            src_ref=time_out.at[w, d, part_of(p, TIME_CHUNK)], dst_ref=time_in.at[w, d, part_of(p, TIME_CHUNK)],
            send_sem=send_sem.at[1], recv_sem=time_sem.at[lax.rem(w, 2), d, p],
            device_id=peer("ta", 2 * d - 1), device_id_type=MESH,
        )

    def load_field(ref, p):
        return unflat([ref[p, i] for i in range(24)], 4)

    def send_time(f, w, p, par, held=False):
        for i, v in enumerate(flat(project(f, 3, -par))):
            time_out[w, 0, p, i] = v
        for i, v in enumerate(flat(link_times(link, 3, project(f, 3, par), True))):
            time_out[w, 1, p, i] = v
        if held:
            pl.when(p < PAIRS - 1)(lambda: start_time(w, p))
        else:
            start_time(w, p)

    def start_time(w, p):
        last = jnp.where(me["ta"] == n_of["ta"] - 1, 1, 0)
        for d in (last, 1 - last):
            time_copy(w, d, p).start()

    def send_edges(f, w, p, par):
        for kind, mu in ((0, 1), (1, 2)):
            for i, v in enumerate(sh.pack(flat(project(f, mu, -par)), kind, True)):
                edge_out[w, 2 * kind, p, i] = v
            start_last(edge_copy, w, 2 * kind, p, EDGE_CHUNK)
            behind = flat(link_times(link, mu, project(f, mu, par), True))
            for i, v in enumerate(behind):
                carried[kind, p, i] = v
            for i, v in enumerate(sh.pack(behind, kind, False)):
                edge_out[w, 2 * kind + 1, p, i] = v
            start_last(edge_copy, w, 2 * kind + 1, p, EDGE_CHUNK)

    def interior(src, par, first=0, end=PAIRS):
        def body(p, _):
            f = load_field(src, p)
            zero = jnp.zeros((8, 128), jnp.float32)
            total = [[(zero, zero)] * 3 for _ in range(4)]
            ahead = unflat(sh.along_x(flat(project(f, 0, -par)), True), 2)
            lift_add(total, link_times(link, 0, ahead, False), 0, -par)
            behind = flat(link_times(link, 0, project(f, 0, par), True))
            lift_add(total, unflat(sh.along_x(behind, False), 2), 0, par)
            for i, v in enumerate(flat(total)):
                acc[p, i] = v
            return _
        lax.fori_loop(first, end, body, 0)

    def receive_body(src, w, p, par):
        await_first(edge_copy, w, p, EDGE_CHUNK, range(4))
        await_first(time_copy, w, p, TIME_CHUNK, range(2))
        f = load_field(src, p)
        total = load_field(acc, p)
        for kind, mu in ((0, 1), (1, 2)):
            got = [edge_in[w, 2 * kind, p, i] for i in range(3)]
            ahead = unflat(sh.shift(flat(project(f, mu, -par)), got, kind, True), 2)
            lift_add(total, link_times(link, mu, ahead, False), mu, -par)
            got = [edge_in[w, 2 * kind + 1, p, i] for i in range(3)]
            local = [carried[kind, p, i] for i in range(12)]
            lift_add(total, unflat(sh.shift(local, got, kind, False), 2), mu, par)
        ahead = unflat([time_in[w, 0, p, i] for i in range(12)], 2)
        lift_add(total, link_times(link, 3, ahead, False), 3, -par)
        lift_add(total, unflat([time_in[w, 1, p, i] for i in range(12)], 2), 3, par)
        return [a - HOP * b for a, b in zip(flat(f), flat(total))]

    def block_copy(slot, gz, device, to):
        return pltpu.make_async_remote_copy(
            src_ref=blocks.at[slot * n_gz + gz], dst_ref=blocks.at[to * n_gz + gz],
            send_sem=send_sem.at[2], recv_sem=block_sem.at[to * n_gz + gz],
            device_id=device, device_id_type=MESH,
        )

    mate = 1 - 2 * lax.rem(me["gz"], 2)
    direct = [(slot, z) for z in range(0, n_gz, 2) for slot in range(reach) if (slot, z) != (own, 0)]

    def send_blocks():
        block_copy(own, me["gz"], across(0, mate), own).start()
        for slot, z in direct:
            block_copy(own, me["gz"], across(own - slot, z), slot).start()

    def pass_blocks():
        for slot, z in direct:
            copy = block_copy(slot, lax.rem(me["gz"] - z + n_gz, n_gz), across(0, mate), slot)
            copy.wait_recv()
            copy.start()

    def await_blocks():
        for z in range(0, n_gz, 2):
            for slot in range(reach):
                block_copy(slot, lax.rem(me["gz"] + mate - z + 2 * n_gz, n_gz), across(0, mate), slot).wait_recv()

    def smt_copy(d):
        return pltpu.make_async_remote_copy(
            src_ref=smt_out.at[d], dst_ref=smt_in.at[d],
            send_sem=send_sem.at[3], recv_sem=smt_sem.at[d],
            device_id=peer("ta", (-1, 1)[d]), device_id_type=MESH,
        )

    def widen(z, _):
        zero = jnp.zeros((8, 128), jnp.float32)
        for g in range(groups):
            for i in range(55):
                wide[g, z, i, 0:4] = blocks[2 * g * n_gz + z, i]
                wide[g, z, i, 4:8] = blocks[(2 * g + 1) * n_gz + z, i]
            for c in range(3):
                for i in range(6):
                    smear[0, g, z, c * 6 + i] = wide[g, z, 0] if i == c else zero
            carry_hops(0, g, z)
        return _

    def links_of(g, z):
        return wide.at[g, z, pl.ds(1, 54)]

    def colour(ref, now, g, z, c):
        return [ref[now, g, z, c * 6 + i] for i in range(6)]

    def carry_hops(now, g, z):
        for c in range(3):
            vector = unflat(colour(smear, now, g, z, c), 1)
            for mu in (2,) if groups == 1 else (2, 1):
                for i, v in enumerate(flat(link_times(links_of(g, z), mu, vector, True))):
                    carry[2 - mu, now, g, z, c * 6 + i] = v

    def beyond(items, others, kind, ahead):
        outs = []
        for v, other in zip(items, others):
            step = -1 if ahead else 1
            inner = (sh.row if kind == 0 else sh.lane // LX)
            last = inner == ((7, 3)[kind] if ahead else 0)
            moved = sh.roll(v, kind, step)
            outs.append(moved if other is None else jnp.where(last, sh.roll(other, kind, step), moved))
        return outs

    def colour_hops(now, g, z, c):
        link_at = links_of(g, z)
        items = colour(smear, now, g, z, c)
        vector = unflat(items, 1)
        out = [(
            flat(link_times(link_at, 0, unflat(sh.along_x(items, True), 1), False)),
            sh.along_x(flat(link_times(link_at, 0, vector, True)), False),
        )]
        if groups == 1:
            later, behind, before = [None] * 6, flat(link_times(link_at, 1, vector, True)), [None] * 6
        else:
            later = colour(smear, now, (g + 1) % groups, z, c)
            behind = colour(carry.at[1], now, g, z, c)
            before = colour(carry.at[1], now, (g - 1) % groups, z, c)
        out.append((
            flat(link_times(link_at, 1, unflat(beyond(items, later, 0, True), 1), False)),
            beyond(behind, before, 0, False),
        ))
        later = colour(smear, now, g, lax.rem(z + 1, n_gz), c)
        behind = colour(carry.at[0], now, g, z, c)
        before = colour(carry.at[0], now, g, lax.rem(z + n_gz - 1, n_gz), c)
        out.append((
            flat(link_times(link_at, 2, unflat(beyond(items, later, 1, True), 1), False)),
            beyond(behind, before, 1, False),
        ))
        return items, out

    def smear_steps(first, end):
        for step in range(first, end):
            now, then = step % 2, (step + 1) % 2
            deep = min(-(-(NSMEAR - step) // (128 // LX)), n_gz // 2)

            def body(k, _):
                z = lax.rem(me["gz"] - deep + k + n_gz, n_gz)
                for g in range(groups):
                    for c in range(3):
                        items, parts = colour_hops(now, g, z, c)
                        for i, v in enumerate(items):
                            total = None
                            for ahead, behind in parts:
                                part = ahead[i] + behind[i]
                                total = part if total is None else total + part
                            smear[then, g, z, c * 6 + i] = (v + 0.25 * total) * 0.5
                    carry_hops(then, g, z)
                return _

            lax.fori_loop(0, min(2 * deep + 1, n_gz), body, 0)

    def both_halves(items):
        return [jnp.where(sh.low, v, pltpu.roll(v, 4, 0)) for v in items]

    def start_right(items):
        carried_on = flat(link_times(link, 3, unflat(items, 1), True))
        for d, values in enumerate((items, carried_on)):
            for a in range(3):
                smt_out[d, a] = jnp.where(sh.low, values[a], values[3 + a])
            smt_copy(d).start()

    def from_time(d):
        smt_copy(d).wait_recv()
        got = [smt_in[d, a] for a in range(3)]
        turned = [pltpu.roll(v, 4, 0) for v in got]
        real = [jnp.where(sh.low, v, t) for v, t in zip(got, turned)]
        return real + [jnp.where(sh.low, t, v) for v, t in zip(got, turned)]

    def take(mu, items, ahead, behind):
        for i in range(6):
            hops[mu, i] = HOP * (behind[i] - ahead[i])
            part = HOP * (ahead[i] + behind[i])
            hops[4, i] = items[i] - part if mu == 0 else hops[4, i] - part

    def local_right(items):
        parts = colour_hops(NSMEAR % 2, own // 2, me["gz"], 0)[1]
        for mu in range(3):
            take(mu, items, *(both_halves(side) for side in parts[mu]))

    def finish_right():
        take(3, None, flat(link_times(link, 3, unflat(from_time(0), 1), False)), from_time(1))
        zero = jnp.zeros((8, 128), jnp.float32)

        def pick(which, a):
            return hops[which, a], hops[which, 3 + a]

        def block(s2, s, a):
            if s2 == s:
                return pick(4, a)
            if s2 // 2 == s // 2:
                return (zero, zero)
            out = (zero, zero)
            for mu in range(4):
                for row in range(2):
                    column, coef = E_ROWS[mu][row]
                    if s2 < 2 and row == s2 and column == s - 2:
                        out = add_term(out, coef, pick(mu, a))
                    if s2 >= 2 and column == s2 - 2 and row == s:
                        out = add_term(out, complex(coef).conjugate(), pick(mu, a))
            return out

        for h in range(2):
            for s2 in range(4):
                for a in range(3):
                    up, down = (block(s2, 2 * h + k, a) for k in range(2))
                    for part in range(2):
                        right[h, part * 12 + s2 * 3 + a] = jnp.where(sh.low, up[part], down[part])

    def first_time(p, _):
        load_guess(p, 0)
        send_time(load_field(guess, p), 0, p, 1)
        return _

    def first_edges(p, _):
        send_edges(load_field(guess, p), 0, p, 1)
        return _

    def give(ref, p, out):
        first, second_rhs = rhs_of(p)
        for i, v in enumerate(out):
            place = pl.ds(4 * (i % 2), 4)
            ref[first, i // 2, place] = v[0:4]
            ref[second_rhs, i // 2, place] = v[4:8]

    def second(p, _):
        out = receive_body(guess, 0, p, 1)
        for i, v in enumerate(out):
            field_a[p, i] = v
        send_time(unflat(out, 4), 1, p, -1)
        send_edges(unflat(out, 4), 1, p, -1)
        return _

    def second_late(p, _):
        spin = 2 * lax.rem(p, 2) + jnp.where(sh.low, 0, 1)
        out = receive_body(guess, 0, p, 1)
        for part in range(2):
            for s2 in range(4):
                for a in range(3):
                    i = part * 12 + s2 * 3 + a
                    source = jnp.where(spin == s2, sources[p // 2, part * 3 + a], 0.0)
                    out[i] = out[i] - source
        for i, v in enumerate(out):
            field_a[p, i] = v
        send_time(unflat(out, 4), 1, p, -1)
        send_edges(unflat(out, 4), 1, p, -1)
        return _

    def no_right(p, _):
        for i in range(24):
            right[p, i] = jnp.zeros((8, 128), jnp.float32)
        return _

    def third(p, _):
        out = [right[p, i] - v for i, v in enumerate(receive_body(field_a, 1, p, -1))]
        total = None
        for i, v in enumerate(out):
            search[p, i] = v
            total = v * v if total is None else total + v * v
        sums[p] = total
        give(search_ref, p, out)
        send_time(unflat(out, 4), 2, p, 1)
        send_edges(unflat(out, 4), 2, p, 1)
        return _

    def run(body, first, end):
        lax.fori_loop(first, end, body, 0)

    send_blocks()
    run(first_time, 0, PAIRS)
    double_links(0, 54)
    run(first_edges, 0, PAIRS)
    interior(guess, 1)
    pass_blocks()
    run(second, 0, 2)
    await_blocks()
    lax.fori_loop(0, n_gz, widen, 0)
    smear_steps(0, NSMEAR)
    for c in range(3):
        for i, v in enumerate(both_halves(colour(smear, NSMEAR % 2, own // 2, me["gz"], c))):
            sources[c, i] = v
    items = [sources[0, i] for i in range(6)]
    start_right(items)
    run(second_late, 2, PAIRS)
    local_right(items)
    interior(field_a, -1)
    run(no_right, 2, PAIRS)
    finish_right()

    run(third, 0, PAIRS)
    interior(search, 1)

    def fourth(p, _):
        out = receive_body(search, 2, p, 1)
        total = None
        for i, v in enumerate(out):
            field_b[p, i] = v
            total = v * v if total is None else total + v * v
        sums[PAIRS + p] = total
        send_time(unflat(out, 4), 3, p, -1, held=True)
        send_edges(unflat(out, 4), 3, p, -1)
        return _

    run(fourth, 0, PAIRS)

    def normal_of(p, _):
        give(normal_ref, p, receive_body(field_b, 3, p, -1))
        return _

    mine = jnp.zeros((8, 128), jnp.float32)
    for k in range(2 * PAIRS):
        mine = jnp.where(sh.lane == k, jnp.sum(sums[k], axis=1, keepdims=True), mine)
    slot = 0
    for stage, axis in enumerate(AXES):
        red_out[stage] = mine
        copies = []
        for k in range(1, n_of[axis]):
            copy = pltpu.make_async_remote_copy(
                src_ref=red_out.at[stage], dst_ref=red_in.at[slot],
                send_sem=send_sem.at[4], recv_sem=red_sem.at[slot],
                device_id=peer(axis, k), device_id_type=MESH,
            )
            copy.start()
            copies.append((copy, slot))
            slot += 1
        if stage == 0:
            interior(field_b, -1)
        if stage == 2:
            start_time(3, PAIRS - 1)
            run(normal_of, 0, PAIRS - 1)
        for copy, place in copies:
            copy.wait_recv()
            mine = mine + red_in[place]
    top = jnp.sum(mine[0:4], axis=0, keepdims=True)
    bottom = jnp.sum(mine[4:8], axis=0, keepdims=True)
    both = jnp.where(sh.low, top, bottom)
    curvature = pltpu.roll(both, 128 - PAIRS, 1)
    steps = both / jnp.where(sh.lane < PAIRS, curvature, 1.0)

    run(normal_of, PAIRS - 1, PAIRS)
    for p in range(PAIRS):
        length = jnp.sum(jnp.where(sh.lane == p, steps, 0.0), axis=1, keepdims=True)
        first = 6 * (p % 2) + p // 2
        second_rhs = first + 3
        length_ref[first : first + 1] = jnp.broadcast_to(length[0:1], (1, 128))
        length_ref[second_rhs : second_rhs + 1] = jnp.broadcast_to(length[4:5], (1, 128))

    passed = blocks.at[pl.ds(0, reach * n_gz - 1)]
    for k, (sent, landed) in enumerate((
        (edge_out, edge_in), (time_out, time_in), (passed, passed), (smt_out, smt_in), (red_in, red_in),
    )):
        pltpu.make_async_remote_copy(
            src_ref=sent, dst_ref=landed, send_sem=send_sem.at[k], recv_sem=red_sem.at[0],
            device_id=peer("ta", 1), device_id_type=MESH,
        ).wait_send()


def on_device(sizes, links, guess, source_sites):
    rows, lanes = guess.shape[-2:]
    f32 = jnp.float32
    copies = sum(n - 1 for n in sizes)
    n_gz = sizes[AXES.index("gz")]
    reach = min(sizes[0], 8)
    groups = reach // 2
    tile = (8, lanes)
    vm = lambda *shape: pltpu.VMEM(shape + tile, f32)
    dma = lambda *shape: pltpu.SemaphoreType.DMA(shape)
    out = jax.ShapeDtypeStruct((12, 12, 2 * rows, lanes), f32)
    search, normal, length = pl.pallas_call(
        functools.partial(kernel, sizes),
        out_shape=(out, out, jax.ShapeDtypeStruct((12, lanes), f32)),
        in_specs=[
            pl.BlockSpec(memory_space=pltpu.HBM),
            pl.BlockSpec(memory_space=pltpu.HBM),
            pl.BlockSpec(memory_space=pltpu.HBM),
        ],
        out_specs=(pl.BlockSpec(memory_space=pltpu.VMEM),) * 3,
        scratch_shapes=[
            pltpu.SMEM((4,), jnp.int32), pltpu.VMEM((72, rows, lanes), f32), pltpu.VMEM((12, 24, rows, lanes), f32),
            pltpu.VMEM((reach * n_gz, 55, rows, lanes), f32), vm(groups, n_gz, 55),
            vm(2, groups, n_gz, 18), vm(min(groups, 2), 2, groups, n_gz, 18),
            vm(72), vm(PAIRS, 24), vm(PAIRS, 24), vm(PAIRS, 24), vm(PAIRS, 24), vm(PAIRS, 24),
            vm(PAIRS, 24), vm(2, PAIRS, 12),
            vm(4, 4, PAIRS, 3), vm(4, 4, PAIRS, 3), vm(4, 2, PAIRS, 12), vm(4, 2, PAIRS, 12),
            vm(2, 3), vm(2, 3),
            vm(3), vm(copies), vm(2 * PAIRS), vm(5, 6), vm(3, 6),
            dma(4), dma(2, 4, PAIRS // EDGE_CHUNK), dma(2, 2, PAIRS), dma(reach * n_gz), dma(2), dma(copies), dma(5),
        ],
        compiler_params=pltpu.CompilerParams(
            collective_id=0, has_side_effects=True, vmem_limit_bytes=48 * 1024 * 1024
        ),
    )(*(
        pltpu.with_memory_space_constraint(x, pltpu.HBM)
        for x in (
            source_sites.reshape(4), links.reshape(72, rows, lanes), guess.reshape(12, 24, rows, lanes)
        )
    ))
    length = length[:, None, None]
    sol = guess.reshape(search.shape) + length * search
    res = search - length * normal
    return sol.reshape(guess.shape), res.reshape(guess.shape)


def solution(mesh):
    sizes = tuple(mesh.shape[axis] for axis in AXES)
    fields = P(None, None, None, None, "ta", "xy", "gz")
    return jax.shard_map(
        functools.partial(on_device, sizes),
        mesh=mesh,
        in_specs=(fields, fields, P("ta", "xy", "gz", None)),
        out_specs=(fields, fields),
        check_vma=False,
    )
```

```python
import functools

import jax
import jax.numpy as jnp
from jax import lax
from jax.experimental import pallas as pl
from jax.experimental.pallas import tpu as pltpu
from jax.sharding import PartitionSpec as P

LX = 32
NSMEAR = 8
HOP = 0.12
PAIRS = 6
EDGE_CHUNK = 3
TIME_CHUNK = 1
MESH = pl.DeviceIdType.MESH
AXES = ("xy", "gz", "ta")

E_ROWS = (
    ((1, -1j), (0, -1j)),
    ((1, -1), (0, 1)),
    ((0, -1j), (1, 1j)),
    ((0, 1), (1, 1)),
)


def times(coef, z):
    re, im = z
    if coef == 1:
        return (1, re), (1, im)
    if coef == -1:
        return (-1, re), (-1, im)
    if coef == 1j:
        return (-1, im), (1, re)
    return (1, im), (-1, re)


def add_term(z, coef, other):
    out = []
    for base, (sign, term) in zip(z, times(coef, other)):
        out.append(base + term if sign > 0 else base - term)
    return tuple(out)


def project(f, mu, parity):
    half = []
    for row in range(2):
        column, coef = E_ROWS[mu][row]
        half.append([add_term(f[row][a], parity * coef, f[2 + column][a]) for a in range(3)])
    return half


def lift_add(total, h, mu, parity):
    for row in range(2):
        column, coef = E_ROWS[mu][row]
        for a in range(3):
            total[row][a] = add_term(total[row][a], 1, h[row][a])
            low = parity * complex(coef).conjugate()
            total[2 + column][a] = add_term(total[2 + column][a], low, h[row][a])


def link_times(link, mu, vectors, adjoint):
    def entry(a, b):
        if adjoint:
            a, b = b, a
        base = mu * 18 + a * 3 + b
        return link[base], link[base + 9]

    out = [[None] * 3 for _ in vectors]
    for a in range(3):
        totals = [None] * len(vectors)
        for b in range(3):
            ur, ui = entry(a, b)
            for k, vec in enumerate(vectors):
                re, im = vec[b]
                if adjoint:
                    tr, ti = ur * re + ui * im, ur * im - ui * re
                else:
                    tr, ti = ur * re - ui * im, ur * im + ui * re
                old = totals[k]
                totals[k] = (tr, ti) if old is None else (old[0] + tr, old[1] + ti)
        for k in range(len(vectors)):
            out[k][a] = totals[k]
    return out


def flat(vectors):
    return [vec[a][part] for part in range(2) for vec in vectors for a in range(3)]


def unflat(items, count):
    return [
        [(items[k * 3 + a], items[3 * count + k * 3 + a]) for a in range(3)] for k in range(count)
    ]


class Shifts:
    def __init__(self):
        row = lax.broadcasted_iota(jnp.int32, (8, 128), 0)
        lane = lax.broadcasted_iota(jnp.int32, (8, 128), 1)
        self.low = row < 4
        self.row = row
        self.lane = lane
        self.place = ([row % 4 == k for k in range(4)], [lane // LX == k for k in range(4)])
        self.x_first = lane % LX == 0
        self.x_last = lane % LX == LX - 1
        self.unit = ((0, 1, 8), (1, LX, 128))

    def roll(self, v, kind, steps):
        axis, unit, size = self.unit[kind]
        amount = (steps * unit) % size
        return v if amount == 0 else pltpu.roll(v, amount, axis)

    def pack(self, items, kind, ahead):
        packed = []
        for g in range(0, len(items), 4):
            out = None
            for k in range(4):
                v = self.roll(items[g + k], kind, k if ahead else k - 3)
                out = v if out is None else jnp.where(self.place[kind][k], v, out)
            packed.append(out)
        return packed

    def shift(self, items, packed, kind, ahead):
        outs = []
        for i, v in enumerate(items):
            got = packed[i // 4]
            k = i % 4
            if ahead:
                moved = self.roll(v, kind, -1)
                outs.append(jnp.where(self.place[kind][3], self.roll(got, kind, 3 - k), moved))
            else:
                moved = self.roll(v, kind, 1)
                outs.append(jnp.where(self.place[kind][0], self.roll(got, kind, -k), moved))
        return outs

    def along_x(self, items, ahead):
        outs = []
        for v in items:
            if ahead:
                a, b = pltpu.roll(v, 127, 1), pltpu.roll(v, LX - 1, 1)
                outs.append(jnp.where(self.x_last, b, a))
            else:
                a, b = pltpu.roll(v, 1, 1), pltpu.roll(v, 129 - LX, 1)
                outs.append(jnp.where(self.x_first, b, a))
        return outs


def kernel(
    sizes, sites_hbm, links_hbm, guess_hbm, search_ref, normal_ref, length_ref,
    sites_ref, links_ref, guess_ref, blocks, wide, smear, carry,
    link, guess, field_a, field_b, search, acc, right, carried,
    edge_out, edge_in, time_out, time_in, smt_out, smt_in,
    red_out, red_in, sums, hops, sources,
    load_sem, edge_sem, time_sem, block_sem, smt_sem, red_sem, send_sem,
):
    n_of = dict(zip(AXES, sizes))
    me = {axis: lax.axis_index(axis) for axis in AXES}
    n_gz = n_of["gz"]
    reach = min(n_of["xy"], 8)
    own = 0 if reach == n_of["xy"] else reach // 2
    groups = reach // 2

    loads = [
        pltpu.make_async_copy(src, dst, load_sem.at[k])
        for k, (src, dst) in enumerate((
            (links_hbm, links_ref), (sites_hbm, sites_ref), (guess_hbm, guess_ref),
            (links_hbm.at[pl.ds(0, 54)], blocks.at[own * n_gz + me["gz"], pl.ds(1, 54)]),
        ))
    ]
    for k in (3, 1, 0, 2):
        loads[k].start()

    def peer(axis, step):
        return {axis: lax.rem(me[axis] + step + n_of[axis], n_of[axis])}

    def across(xy, gz):
        return {
            "xy": lax.rem(me["xy"] + xy + n_of["xy"], n_of["xy"]),
            "gz": lax.rem(me["gz"] + gz + n_gz, n_gz),
        }

    shifts = sorted({(slot - own) % n_of["xy"] for slot in range(reach)} | {(own - slot) % n_of["xy"] for slot in range(reach)})
    greeted = [across(y, z) for y in shifts for z in range(n_gz) if (y, z) != (0, 0)]
    greeted += [peer("xy", y) for y in range(1, n_of["xy"]) if y not in shifts]
    greeted += [peer("ta", t) for t in range(1, n_of["ta"])]
    barrier = pltpu.get_barrier_semaphore()
    for device in greeted:
        pl.semaphore_signal(barrier, inc=1, device_id=device, device_id_type=MESH)

    sh = Shifts()

    row = lax.broadcasted_iota(jnp.int32, (4, 128), 0)
    lane = lax.broadcasted_iota(jnp.int32, (4, 128), 1)
    loads[3].wait()
    loads[1].wait()
    hit = (row == sites_ref[1]) & (lane == sites_ref[2] * LX + sites_ref[3])
    hit = hit & (sites_ref[0] == 0)
    blocks[own * n_gz + me["gz"], 0] = jnp.where(hit, 1.0, 0.0).astype(jnp.float32)

    loads[0].wait()
    sign = jnp.where(me["ta"] == n_of["ta"] - 1, -1.0, 1.0).astype(jnp.float32)

    def double_links(first, end):
        for i in range(first, end):
            v = links_ref[i]
            if i >= 54:
                v = v * sign
            link[i, 0:4, :] = v
            link[i, 4:8, :] = v

    double_links(54, 72)

    def rhs_of(p):
        first = 6 * lax.rem(p, 2) + p // 2
        return first, first + 3

    def load_guess(p, _):
        first, second = rhs_of(p)
        for i in range(24):
            guess[p, i, 0:4, :] = guess_ref[first, i]
            guess[p, i, 4:8, :] = guess_ref[second, i]
        return _

    loads[2].wait()
    pl.semaphore_wait(barrier, len(greeted))

    def part_of(p, chunk):
        return pl.ds(p, chunk)

    def start_last(make, w, d, p, chunk):
        if chunk == 1:
            make(w, d, p).start()
        else:
            @pl.when(lax.rem(p, chunk) == chunk - 1)
            def _():
                make(w, d, p - (chunk - 1)).start()

    def edge_copy(w, d, p):
        axis, step = (("xy", -1), ("xy", 1), ("gz", -1), ("gz", 1))[0 if isinstance(d, slice) else d]
        return pltpu.make_async_remote_copy(
            src_ref=edge_out.at[w, d, part_of(p, EDGE_CHUNK)], dst_ref=edge_in.at[w, d, part_of(p, EDGE_CHUNK)],
            send_sem=send_sem.at[0], recv_sem=edge_sem.at[lax.rem(w, 2), p // EDGE_CHUNK],
            device_id=peer(axis, step), device_id_type=MESH,
        )

    def time_copy(w, d, p):
        return pltpu.make_async_remote_copy(
            src_ref=time_out.at[w, d, part_of(p, TIME_CHUNK)], dst_ref=time_in.at[w, d, part_of(p, TIME_CHUNK)],
            send_sem=send_sem.at[1], recv_sem=time_sem.at[lax.rem(w, 2), p],
            device_id=peer("ta", 1 if isinstance(d, slice) else 2 * d - 1), device_id_type=MESH,
        )

    def await_edges(w, p):
        def wait():
            edge_copy(w, slice(None), p).wait_recv()

        pl.when(lax.rem(p, EDGE_CHUNK) == 0)(wait)

    def await_time(w, p):
        time_copy(w, slice(None), p).wait_recv()

    def load_field(ref, p):
        return unflat([ref[p, i] for i in range(24)], 4)

    def send_time(f, w, p, par, held=False):
        for i, v in enumerate(flat(project(f, 3, -par))):
            time_out[w, 0, p, i] = v
        for i, v in enumerate(flat(link_times(link, 3, project(f, 3, par), True))):
            time_out[w, 1, p, i] = v
        if held:
            pl.when(p < PAIRS - 1)(lambda: start_time(w, p))
        else:
            start_time(w, p)

    def start_time(w, p):
        last = jnp.where(me["ta"] == n_of["ta"] - 1, 1, 0)
        for d in (last, 1 - last):
            time_copy(w, d, p).start()

    def send_edges(f, w, p, par):
        for kind, mu in ((0, 1), (1, 2)):
            for i, v in enumerate(sh.pack(flat(project(f, mu, -par)), kind, True)):
                edge_out[w, 2 * kind, p, i] = v
            start_last(edge_copy, w, 2 * kind, p, EDGE_CHUNK)
            behind = flat(link_times(link, mu, project(f, mu, par), True))
            for i, v in enumerate(behind):
                carried[kind, p, i] = v
            for i, v in enumerate(sh.pack(behind, kind, False)):
                edge_out[w, 2 * kind + 1, p, i] = v
            start_last(edge_copy, w, 2 * kind + 1, p, EDGE_CHUNK)

    def interior(src, par, first=0, end=PAIRS):
        def body(p, _):
            f = load_field(src, p)
            zero = jnp.zeros((8, 128), jnp.float32)
            total = [[(zero, zero)] * 3 for _ in range(4)]
            ahead = unflat(sh.along_x(flat(project(f, 0, -par)), True), 2)
            lift_add(total, link_times(link, 0, ahead, False), 0, -par)
            behind = flat(link_times(link, 0, project(f, 0, par), True))
            lift_add(total, unflat(sh.along_x(behind, False), 2), 0, par)
            for i, v in enumerate(flat(total)):
                acc[p, i] = v
            return _
        lax.fori_loop(first, end, body, 0)

    def receive_body(src, w, p, par):
        await_edges(w, p)
        await_time(w, p)
        f = load_field(src, p)
        total = load_field(acc, p)
        for kind, mu in ((0, 1), (1, 2)):
            got = [edge_in[w, 2 * kind, p, i] for i in range(3)]
            ahead = unflat(sh.shift(flat(project(f, mu, -par)), got, kind, True), 2)
            lift_add(total, link_times(link, mu, ahead, False), mu, -par)
            got = [edge_in[w, 2 * kind + 1, p, i] for i in range(3)]
            local = [carried[kind, p, i] for i in range(12)]
            lift_add(total, unflat(sh.shift(local, got, kind, False), 2), mu, par)
        ahead = unflat([time_in[w, 0, p, i] for i in range(12)], 2)
        lift_add(total, link_times(link, 3, ahead, False), 3, -par)
        lift_add(total, unflat([time_in[w, 1, p, i] for i in range(12)], 2), 3, par)
        return [a - HOP * b for a, b in zip(flat(f), flat(total))]

    def block_copy(slot, gz, device, to):
        return pltpu.make_async_remote_copy(
            src_ref=blocks.at[slot * n_gz + gz], dst_ref=blocks.at[to * n_gz + gz],
            send_sem=send_sem.at[2], recv_sem=block_sem.at[to * n_gz + gz],
            device_id=device, device_id_type=MESH,
        )

    mate = 1 - 2 * lax.rem(me["gz"], 2)
    direct = [(slot, z) for z in range(0, n_gz, 2) for slot in range(reach) if (slot, z) != (own, 0)]

    def send_blocks():
        block_copy(own, me["gz"], across(0, mate), own).start()
        for slot, z in direct:
            block_copy(own, me["gz"], across(own - slot, z), slot).start()

    def pass_blocks():
        for slot, z in direct:
            copy = block_copy(slot, lax.rem(me["gz"] - z + n_gz, n_gz), across(0, mate), slot)
            copy.wait_recv()
            copy.start()

    def await_blocks():
        for z in range(0, n_gz, 2):
            for slot in range(reach):
                block_copy(slot, lax.rem(me["gz"] + mate - z + 2 * n_gz, n_gz), across(0, mate), slot).wait_recv()

    def smt_copy(d):
        return pltpu.make_async_remote_copy(
            src_ref=smt_out.at[d], dst_ref=smt_in.at[d],
            send_sem=send_sem.at[3], recv_sem=smt_sem.at[0],
            device_id=peer("ta", 1 if isinstance(d, slice) else 2 * d - 1), device_id_type=MESH,
        )

    def widen(z, _):
        for g in range(groups):
            for i in range(55):
                wide[g, z, i, 0:4] = blocks[2 * g * n_gz + z, i]
                wide[g, z, i, 4:8] = blocks[(2 * g + 1) * n_gz + z, i]
        return _

    def links_of(g, z):
        return wide.at[g, z, pl.ds(1, 54)]

    def colour(ref, now, g, z, c):
        return [ref[now, g, z, c * 6 + i] for i in range(6)]

    def carry_hops(now, g, z):
        for c in range(3):
            vector = unflat(colour(smear, now, g, z, c), 1)
            for mu in (2,) if groups == 1 else (2, 1):
                for i, v in enumerate(flat(link_times(links_of(g, z), mu, vector, True))):
                    carry[2 - mu, now, g, z, c * 6 + i] = v

    def beyond(items, others, kind, ahead):
        outs = []
        for v, other in zip(items, others):
            step = -1 if ahead else 1
            inner = (sh.row if kind == 0 else sh.lane // LX)
            last = inner == ((7, 3)[kind] if ahead else 0)
            moved = sh.roll(v, kind, step)
            outs.append(moved if other is None else jnp.where(last, sh.roll(other, kind, step), moved))
        return outs

    def colour_hops(now, g, z, c):
        link_at = links_of(g, z)
        items = colour(smear, now, g, z, c)
        vector = unflat(items, 1)
        out = [(
            flat(link_times(link_at, 0, unflat(sh.along_x(items, True), 1), False)),
            sh.along_x(flat(link_times(link_at, 0, vector, True)), False),
        )]
        if groups == 1:
            later, behind, before = [None] * 6, flat(link_times(link_at, 1, vector, True)), [None] * 6
        else:
            later = colour(smear, now, (g + 1) % groups, z, c)
            behind = colour(carry.at[1], now, g, z, c)
            before = colour(carry.at[1], now, (g - 1) % groups, z, c)
        out.append((
            flat(link_times(link_at, 1, unflat(beyond(items, later, 0, True), 1), False)),
            beyond(behind, before, 0, False),
        ))
        later = colour(smear, now, g, lax.rem(z + 1, n_gz), c)
        behind = colour(carry.at[0], now, g, z, c)
        before = colour(carry.at[0], now, g, lax.rem(z + n_gz - 1, n_gz), c)
        out.append((
            flat(link_times(link_at, 2, unflat(beyond(items, later, 1, True), 1), False)),
            beyond(behind, before, 1, False),
        ))
        return items, out

    def from_points(g, z):
        point = wide[g, z, 0]
        return [
            [[(wide[g, z, 1 + mu * 18 + c * 3 + a] * point, wide[g, z, 10 + mu * 18 + c * 3 + a] * -point)
              for a in range(3)] for c in range(3)]
            for mu in range(3)
        ]

    def first_step(k, _):
        z = lax.rem(me["gz"] + k, n_gz)
        for g in range(groups):
            point = wide[g, z, 0]
            after, before = lax.rem(z + 1, n_gz), lax.rem(z + n_gz - 1, n_gz)
            up = None if groups == 1 else wide[(g + 1) % groups, z, 0]
            ahead = [
                sh.along_x([point], True)[0], beyond([point], [up], 0, True)[0],
                beyond([point], [wide[g, after, 0]], 1, True)[0],
            ]
            back = from_points(g, z)
            below = None if groups == 1 else from_points((g - 1) % groups, z)
            beside = from_points(g, before)
            for c in range(3):
                sides = [
                    sh.along_x(flat([back[0][c]]), False),
                    beyond(flat([back[1][c]]), [None] * 6 if groups == 1 else flat([below[1][c]]), 0, False),
                    beyond(flat([back[2][c]]), flat([beside[2][c]]), 1, False),
                ]
                for part in range(2):
                    for a in range(3):
                        i = part * 3 + a
                        total = None
                        for mu in range(3):
                            term = wide[g, z, 1 + mu * 18 + part * 9 + a * 3 + c] * ahead[mu] + sides[mu][i]
                            total = term if total is None else total + term
                        value = 0.25 * total if i != c else point + 0.25 * total
                        smear[1, g, z, c * 6 + i] = value * 0.5
            carry_hops(1, g, z)
        return _

    def smear_steps(first, end):
        for step in range(first, end):
            now, then = step % 2, (step + 1) % 2
            deep = min(-(-(NSMEAR - step) // (128 // LX)), n_gz // 2)

            def body(k, _):
                z = lax.rem(me["gz"] - deep + k + n_gz, n_gz)
                for g in range(groups):
                    for c in range(3):
                        items, parts = colour_hops(now, g, z, c)
                        for i, v in enumerate(items):
                            total = None
                            for ahead, behind in parts:
                                part = ahead[i] + behind[i]
                                total = part if total is None else total + part
                            smear[then, g, z, c * 6 + i] = (v + 0.25 * total) * 0.5
                    carry_hops(then, g, z)
                return _

            lax.fori_loop(0, min(2 * deep + 1, n_gz), body, 0)

    def both_halves(items):
        return [jnp.where(sh.low, v, pltpu.roll(v, 4, 0)) for v in items]

    def start_right(items):
        carried_on = flat(link_times(link, 3, unflat(items, 1), True))
        for d, values in enumerate((items, carried_on)):
            for a in range(3):
                smt_out[d, a] = jnp.where(sh.low, values[a], values[3 + a])
            smt_copy(d).start()

    def from_time(d):
        got = [smt_in[d, a] for a in range(3)]
        turned = [pltpu.roll(v, 4, 0) for v in got]
        real = [jnp.where(sh.low, v, t) for v, t in zip(got, turned)]
        return real + [jnp.where(sh.low, t, v) for v, t in zip(got, turned)]

    def take(mu, items, ahead, behind):
        for i in range(6):
            hops[mu, i] = HOP * (behind[i] - ahead[i])
            part = HOP * (ahead[i] + behind[i])
            hops[4, i] = items[i] - part if mu == 0 else hops[4, i] - part

    def local_right(items):
        parts = colour_hops(NSMEAR % 2, own // 2, me["gz"], 0)[1]
        for mu in range(3):
            take(mu, items, *(both_halves(side) for side in parts[mu]))

    def finish_right():
        smt_copy(slice(None)).wait_recv()
        take(3, None, flat(link_times(link, 3, unflat(from_time(0), 1), False)), from_time(1))
        zero = jnp.zeros((8, 128), jnp.float32)

        def pick(which, a):
            return hops[which, a], hops[which, 3 + a]

        def block(s2, s, a):
            if s2 == s:
                return pick(4, a)
            if s2 // 2 == s // 2:
                return (zero, zero)
            out = (zero, zero)
            for mu in range(4):
                for row in range(2):
                    column, coef = E_ROWS[mu][row]
                    if s2 < 2 and row == s2 and column == s - 2:
                        out = add_term(out, coef, pick(mu, a))
                    if s2 >= 2 and column == s2 - 2 and row == s:
                        out = add_term(out, complex(coef).conjugate(), pick(mu, a))
            return out

        for h in range(2):
            for s2 in range(4):
                for a in range(3):
                    up, down = (block(s2, 2 * h + k, a) for k in range(2))
                    for part in range(2):
                        right[h, part * 12 + s2 * 3 + a] = jnp.where(sh.low, up[part], down[part])

    def first_time(p, _):
        load_guess(p, 0)
        send_time(load_field(guess, p), 0, p, 1)
        return _

    def first_edges(p, _):
        send_edges(load_field(guess, p), 0, p, 1)
        return _

    def give(ref, p, out):
        first, second_rhs = rhs_of(p)
        for i, v in enumerate(out):
            place = pl.ds(4 * (i % 2), 4)
            ref[first, i // 2, place] = v[0:4]
            ref[second_rhs, i // 2, place] = v[4:8]

    def second(p, _):
        out = receive_body(guess, 0, p, 1)
        for i, v in enumerate(out):
            field_a[p, i] = v
        send_time(unflat(out, 4), 1, p, -1)
        send_edges(unflat(out, 4), 1, p, -1)
        return _

    def second_late(p, _):
        spin = 2 * lax.rem(p, 2) + jnp.where(sh.low, 0, 1)
        out = receive_body(guess, 0, p, 1)
        for part in range(2):
            for s2 in range(4):
                for a in range(3):
                    i = part * 12 + s2 * 3 + a
                    source = jnp.where(spin == s2, sources[p // 2, part * 3 + a], 0.0)
                    out[i] = out[i] - source
        for i, v in enumerate(out):
            field_a[p, i] = v
        send_time(unflat(out, 4), 1, p, -1)
        send_edges(unflat(out, 4), 1, p, -1)
        return _

    def no_right(p, _):
        for i in range(24):
            right[p, i] = jnp.zeros((8, 128), jnp.float32)
        return _

    def third(p, _):
        out = [right[p, i] - v for i, v in enumerate(receive_body(field_a, 1, p, -1))]
        total = None
        for i, v in enumerate(out):
            search[p, i] = v
            total = v * v if total is None else total + v * v
        sums[p] = total
        give(search_ref, p, out)
        send_time(unflat(out, 4), 2, p, 1)
        send_edges(unflat(out, 4), 2, p, 1)
        return _

    def run(body, first, end):
        lax.fori_loop(first, end, body, 0)

    send_blocks()
    run(first_time, 0, PAIRS)
    double_links(0, 54)
    run(first_edges, 0, PAIRS)
    interior(guess, 1)
    pass_blocks()
    run(second, 0, 1)
    await_blocks()
    lax.fori_loop(0, n_gz, widen, 0)
    lax.fori_loop(0, n_gz, first_step, 0)
    smear_steps(1, 3)
    run(second, 1, 2)
    smear_steps(3, NSMEAR)
    for c in range(3):
        for i, v in enumerate(both_halves(colour(smear, NSMEAR % 2, own // 2, me["gz"], c))):
            sources[c, i] = v
    items = [sources[0, i] for i in range(6)]
    start_right(items)
    run(second_late, 2, PAIRS)
    local_right(items)
    interior(field_a, -1)
    run(no_right, 2, PAIRS)
    finish_right()

    run(third, 0, PAIRS)
    interior(search, 1)

    def fourth(p, _):
        out = receive_body(search, 2, p, 1)
        total = None
        for i, v in enumerate(out):
            field_b[p, i] = v
            total = v * v if total is None else total + v * v
        sums[PAIRS + p] = total
        send_time(unflat(out, 4), 3, p, -1, held=True)
        send_edges(unflat(out, 4), 3, p, -1)
        return _

    run(fourth, 0, PAIRS)

    def normal_of(p, _):
        give(normal_ref, p, receive_body(field_b, 3, p, -1))
        return _

    mine = jnp.zeros((8, 128), jnp.float32)
    for k in range(2 * PAIRS):
        mine = jnp.where(sh.lane == k, jnp.sum(sums[k], axis=1, keepdims=True), mine)
    slot = 0
    for stage, axis in enumerate(AXES):
        red_out[stage] = mine
        others = n_of[axis] - 1

        def sum_copy(k, place):
            return pltpu.make_async_remote_copy(
                src_ref=red_out.at[stage], dst_ref=red_in.at[place],
                send_sem=send_sem.at[4], recv_sem=red_sem.at[stage],
                device_id=peer(axis, k), device_id_type=MESH,
            )

        for k in range(1, others + 1):
            sum_copy(k, slot + k - 1).start()
        if stage == 0:
            interior(field_b, -1)
        if stage == 2:
            start_time(3, PAIRS - 1)
            run(normal_of, 0, PAIRS - 1)
        landed = red_in.at[pl.ds(slot, others)]
        pltpu.make_async_remote_copy(
            src_ref=landed, dst_ref=landed, send_sem=send_sem.at[4], recv_sem=red_sem.at[stage],
            device_id=peer(axis, 1), device_id_type=MESH,
        ).wait_recv()
        for k in range(others):
            mine = mine + red_in[slot + k]
        slot += others
    top = jnp.sum(mine[0:4], axis=0, keepdims=True)
    bottom = jnp.sum(mine[4:8], axis=0, keepdims=True)
    both = jnp.where(sh.low, top, bottom)
    curvature = pltpu.roll(both, 128 - PAIRS, 1)
    steps = both / jnp.where(sh.lane < PAIRS, curvature, 1.0)

    for p in range(PAIRS):
        length = jnp.sum(jnp.where(sh.lane == p, steps, 0.0), axis=1, keepdims=True)
        first = 6 * (p % 2) + p // 2
        second_rhs = first + 3
        length_ref[first : first + 1] = jnp.broadcast_to(length[0:1], (1, 128))
        length_ref[second_rhs : second_rhs + 1] = jnp.broadcast_to(length[4:5], (1, 128))

    run(normal_of, PAIRS - 1, PAIRS)

    passed = blocks.at[pl.ds(0, reach * n_gz - 1)]
    for k, (sent, landed) in enumerate((
        (edge_out, edge_in), (time_out, time_in), (passed, passed), (smt_out, smt_in), (red_in, red_in),
    )):
        pltpu.make_async_remote_copy(
            src_ref=sent, dst_ref=landed, send_sem=send_sem.at[k], recv_sem=red_sem.at[0],
            device_id=peer("ta", 1), device_id_type=MESH,
        ).wait_send()


def on_device(sizes, links, guess, source_sites):
    rows, lanes = guess.shape[-2:]
    f32 = jnp.float32
    copies = sum(n - 1 for n in sizes)
    n_gz = sizes[AXES.index("gz")]
    reach = min(sizes[0], 8)
    groups = reach // 2
    tile = (8, lanes)
    vm = lambda *shape: pltpu.VMEM(shape + tile, f32)
    dma = lambda *shape: pltpu.SemaphoreType.DMA(shape)
    out = jax.ShapeDtypeStruct((12, 12, 2 * rows, lanes), f32)
    search, normal, length = pl.pallas_call(
        functools.partial(kernel, sizes),
        out_shape=(out, out, jax.ShapeDtypeStruct((12, lanes), f32)),
        in_specs=[
            pl.BlockSpec(memory_space=pltpu.HBM),
            pl.BlockSpec(memory_space=pltpu.HBM),
            pl.BlockSpec(memory_space=pltpu.HBM),
        ],
        out_specs=(pl.BlockSpec(memory_space=pltpu.VMEM),) * 3,
        scratch_shapes=[
            pltpu.SMEM((4,), jnp.int32), pltpu.VMEM((72, rows, lanes), f32), pltpu.VMEM((12, 24, rows, lanes), f32),
            pltpu.VMEM((reach * n_gz, 55, rows, lanes), f32), vm(groups, n_gz, 55),
            vm(2, groups, n_gz, 18), vm(min(groups, 2), 2, groups, n_gz, 18),
            vm(72), vm(PAIRS, 24), vm(PAIRS, 24), vm(PAIRS, 24), vm(PAIRS, 24), vm(PAIRS, 24),
            vm(PAIRS, 24), vm(2, PAIRS, 12),
            vm(4, 4, PAIRS, 3), vm(4, 4, PAIRS, 3), vm(4, 2, PAIRS, 12), vm(4, 2, PAIRS, 12),
            vm(2, 3), vm(2, 3),
            vm(3), vm(copies), vm(2 * PAIRS), vm(5, 6), vm(3, 6),
            dma(4), dma(2, PAIRS // EDGE_CHUNK), dma(2, PAIRS), dma(reach * n_gz), dma(1), dma(3), dma(5),
        ],
        compiler_params=pltpu.CompilerParams(
            collective_id=0, has_side_effects=True, vmem_limit_bytes=48 * 1024 * 1024
        ),
    )(*(
        pltpu.with_memory_space_constraint(x, pltpu.HBM)
        for x in (
            source_sites.reshape(4), links.reshape(72, rows, lanes), guess.reshape(12, 24, rows, lanes)
        )
    ))
    length = length[:, None, None]
    sol = guess.reshape(search.shape) + length * search
    res = search - length * normal
    return sol.reshape(guess.shape), res.reshape(guess.shape)


def solution(mesh):
    sizes = tuple(mesh.shape[axis] for axis in AXES)
    fields = P(None, None, None, None, "ta", "xy", "gz")
    return jax.shard_map(
        functools.partial(on_device, sizes),
        mesh=mesh,
        in_specs=(fields, fields, P("ta", "xy", "gz", None)),
        out_specs=(fields, fields),
        check_vma=False,
    )
```

```python
import functools

import jax
import jax.numpy as jnp
from jax import lax
from jax.experimental import pallas as pl
from jax.experimental.pallas import tpu as pltpu
from jax.sharding import PartitionSpec as P

LX = 32
NSMEAR = 8
HOP = 0.12
PAIRS = 6
EDGE_CHUNK = 3
TIME_CHUNK = 1
MESH = pl.DeviceIdType.MESH
AXES = ("xy", "gz", "ta")

E_ROWS = (
    ((1, -1j), (0, -1j)),
    ((1, -1), (0, 1)),
    ((0, -1j), (1, 1j)),
    ((0, 1), (1, 1)),
)


def times(coef, z):
    re, im = z
    if coef == 1:
        return (1, re), (1, im)
    if coef == -1:
        return (-1, re), (-1, im)
    if coef == 1j:
        return (-1, im), (1, re)
    return (1, im), (-1, re)


def add_term(z, coef, other):
    out = []
    for base, (sign, term) in zip(z, times(coef, other)):
        out.append(base + term if sign > 0 else base - term)
    return tuple(out)


def project(f, mu, parity):
    half = []
    for row in range(2):
        column, coef = E_ROWS[mu][row]
        half.append([add_term(f[row][a], parity * coef, f[2 + column][a]) for a in range(3)])
    return half


def lift_add(total, h, mu, parity):
    for row in range(2):
        column, coef = E_ROWS[mu][row]
        for a in range(3):
            total[row][a] = add_term(total[row][a], 1, h[row][a])
            low = parity * complex(coef).conjugate()
            total[2 + column][a] = add_term(total[2 + column][a], low, h[row][a])


def link_times(link, mu, vectors, adjoint):
    def entry(a, b):
        if adjoint:
            a, b = b, a
        base = mu * 18 + a * 3 + b
        return link[base], link[base + 9]

    out = [[None] * 3 for _ in vectors]
    for a in range(3):
        totals = [None] * len(vectors)
        for b in range(3):
            ur, ui = entry(a, b)
            for k, vec in enumerate(vectors):
                re, im = vec[b]
                if adjoint:
                    tr, ti = ur * re + ui * im, ur * im - ui * re
                else:
                    tr, ti = ur * re - ui * im, ur * im + ui * re
                old = totals[k]
                totals[k] = (tr, ti) if old is None else (old[0] + tr, old[1] + ti)
        for k in range(len(vectors)):
            out[k][a] = totals[k]
    return out


def flat(vectors):
    return [vec[a][part] for part in range(2) for vec in vectors for a in range(3)]


def unflat(items, count):
    return [
        [(items[k * 3 + a], items[3 * count + k * 3 + a]) for a in range(3)] for k in range(count)
    ]


class Shifts:
    def __init__(self):
        row = lax.broadcasted_iota(jnp.int32, (8, 128), 0)
        lane = lax.broadcasted_iota(jnp.int32, (8, 128), 1)
        self.low = row < 4
        self.row = row
        self.lane = lane
        self.place = ([row % 4 == k for k in range(4)], [lane // LX == k for k in range(4)])
        self.x_first = lane % LX == 0
        self.x_last = lane % LX == LX - 1
        self.unit = ((0, 1, 8), (1, LX, 128))

    def roll(self, v, kind, steps):
        axis, unit, size = self.unit[kind]
        amount = (steps * unit) % size
        return v if amount == 0 else pltpu.roll(v, amount, axis)

    def pack(self, items, kind, ahead):
        packed = []
        for g in range(0, len(items), 4):
            out = None
            for k in range(4):
                v = self.roll(items[g + k], kind, k if ahead else k - 3)
                out = v if out is None else jnp.where(self.place[kind][k], v, out)
            packed.append(out)
        return packed

    def shift(self, items, packed, kind, ahead):
        outs = []
        for i, v in enumerate(items):
            got = packed[i // 4]
            k = i % 4
            if ahead:
                moved = self.roll(v, kind, -1)
                outs.append(jnp.where(self.place[kind][3], self.roll(got, kind, 3 - k), moved))
            else:
                moved = self.roll(v, kind, 1)
                outs.append(jnp.where(self.place[kind][0], self.roll(got, kind, -k), moved))
        return outs

    def along_x(self, items, ahead):
        outs = []
        for v in items:
            if ahead:
                a, b = pltpu.roll(v, 127, 1), pltpu.roll(v, LX - 1, 1)
                outs.append(jnp.where(self.x_last, b, a))
            else:
                a, b = pltpu.roll(v, 1, 1), pltpu.roll(v, 129 - LX, 1)
                outs.append(jnp.where(self.x_first, b, a))
        return outs


def kernel(
    sizes, sites_hbm, links_hbm, guess_hbm, search_ref, normal_ref, length_ref,
    sites_ref, links_ref, guess_ref, blocks, wide, smear, carry,
    link, guess, field_a, field_b, search, acc, right, carried,
    edge_out, edge_in, time_out, time_in, smt_out, smt_in,
    red_out, red_in, sums, hops, sources,
    load_sem, edge_sem, time_sem, block_sem, smt_sem, red_sem, send_sem,
):
    n_of = dict(zip(AXES, sizes))
    me = {axis: lax.axis_index(axis) for axis in AXES}
    n_gz = n_of["gz"]
    reach = min(n_of["xy"], 8)
    own = 0 if reach == n_of["xy"] else reach // 2
    groups = reach // 2

    loads = [
        pltpu.make_async_copy(src, dst, load_sem.at[k])
        for k, (src, dst) in enumerate((
            (links_hbm, links_ref), (sites_hbm, sites_ref), (guess_hbm, guess_ref),
            (links_hbm.at[pl.ds(0, 54)], blocks.at[own * n_gz + me["gz"], pl.ds(1, 54)]),
        ))
    ]
    for k in (3, 1, 0, 2):
        loads[k].start()

    def peer(axis, step):
        return {axis: lax.rem(me[axis] + step + n_of[axis], n_of[axis])}

    def across(xy, gz):
        return {
            "xy": lax.rem(me["xy"] + xy + n_of["xy"], n_of["xy"]),
            "gz": lax.rem(me["gz"] + gz + n_gz, n_gz),
        }

    shifts = sorted({(slot - own) % n_of["xy"] for slot in range(reach)} | {(own - slot) % n_of["xy"] for slot in range(reach)})
    greeted = [across(y, z) for y in shifts for z in range(n_gz) if (y, z) != (0, 0)]
    greeted += [peer("xy", y) for y in range(1, n_of["xy"]) if y not in shifts]
    greeted += [peer("ta", t) for t in range(1, n_of["ta"])]
    barrier = pltpu.get_barrier_semaphore()
    for device in greeted:
        pl.semaphore_signal(barrier, inc=1, device_id=device, device_id_type=MESH)

    sh = Shifts()

    row = lax.broadcasted_iota(jnp.int32, (4, 128), 0)
    lane = lax.broadcasted_iota(jnp.int32, (4, 128), 1)
    loads[3].wait()
    loads[1].wait()
    hit = (row == sites_ref[1]) & (lane == sites_ref[2] * LX + sites_ref[3])
    hit = hit & (sites_ref[0] == 0)
    blocks[own * n_gz + me["gz"], 0] = jnp.where(hit, 1.0, 0.0).astype(jnp.float32)

    loads[0].wait()
    sign = jnp.where(me["ta"] == n_of["ta"] - 1, -1.0, 1.0).astype(jnp.float32)

    def double_links(first, end):
        for i in range(first, end):
            v = links_ref[i]
            if i >= 54:
                v = v * sign
            link[i, 0:4, :] = v
            link[i, 4:8, :] = v

    double_links(54, 72)

    def rhs_of(p):
        first = 6 * lax.rem(p, 2) + p // 2
        return first, first + 3

    def load_guess(p, _):
        first, second = rhs_of(p)
        for i in range(24):
            guess[p, i, 0:4, :] = guess_ref[first, i]
            guess[p, i, 4:8, :] = guess_ref[second, i]
        return _

    loads[2].wait()
    pl.semaphore_wait(barrier, len(greeted))

    def part_of(p, chunk):
        return pl.ds(p, chunk)

    def start_last(make, w, d, p, chunk):
        if chunk == 1:
            make(w, d, p).start()
        else:
            @pl.when(lax.rem(p, chunk) == chunk - 1)
            def _():
                make(w, d, p - (chunk - 1)).start()

    def edge_copy(w, d, p):
        axis, step = (("xy", -1), ("xy", 1), ("gz", -1), ("gz", 1))[0 if isinstance(d, slice) else d]
        return pltpu.make_async_remote_copy(
            src_ref=edge_out.at[w, d, part_of(p, EDGE_CHUNK)], dst_ref=edge_in.at[w, d, part_of(p, EDGE_CHUNK)],
            send_sem=send_sem.at[0], recv_sem=edge_sem.at[lax.rem(w, 2), p // EDGE_CHUNK],
            device_id=peer(axis, step), device_id_type=MESH,
        )

    def time_copy(w, d, p):
        return pltpu.make_async_remote_copy(
            src_ref=time_out.at[w, d, part_of(p, TIME_CHUNK)], dst_ref=time_in.at[w, d, part_of(p, TIME_CHUNK)],
            send_sem=send_sem.at[1], recv_sem=time_sem.at[lax.rem(w, 2), p],
            device_id=peer("ta", 1 if isinstance(d, slice) else 2 * d - 1), device_id_type=MESH,
        )

    def await_edges(w, p):
        def wait():
            edge_copy(w, slice(None), p).wait_recv()

        pl.when(lax.rem(p, EDGE_CHUNK) == 0)(wait)

    def await_time(w, p):
        time_copy(w, slice(None), p).wait_recv()

    def load_field(ref, p):
        return unflat([ref[p, i] for i in range(24)], 4)

    first_core = lax.rem(me["gz"], 2) == 0
    other_core = lax.rem(me["gz"], 2) == 1

    def send_time(f, w, p, par, held=False):
        for i, v in enumerate(flat(project(f, 3, -par))):
            time_out[w, 0, p, i] = v
        for i, v in enumerate(flat(link_times(link, 3, project(f, 3, par), True))):
            time_out[w, 1, p, i] = v
        if held:
            pl.when((p < PAIRS - 2) | ((p < PAIRS - 1) & first_core))(lambda: start_time(w, p))
        else:
            start_time(w, p)

    def start_time(w, p):
        last = jnp.where(me["ta"] == n_of["ta"] - 1, 1, 0)
        for d in (last, 1 - last):
            time_copy(w, d, p).start()

    def send_edges(f, w, p, par):
        for kind, mu in ((0, 1), (1, 2)):
            for i, v in enumerate(sh.pack(flat(project(f, mu, -par)), kind, True)):
                edge_out[w, 2 * kind, p, i] = v
            start_last(edge_copy, w, 2 * kind, p, EDGE_CHUNK)
            behind = flat(link_times(link, mu, project(f, mu, par), True))
            for i, v in enumerate(behind):
                carried[kind, p, i] = v
            for i, v in enumerate(sh.pack(behind, kind, False)):
                edge_out[w, 2 * kind + 1, p, i] = v
            start_last(edge_copy, w, 2 * kind + 1, p, EDGE_CHUNK)

    def interior(src, par, first=0, end=PAIRS):
        def body(p, _):
            f = load_field(src, p)
            zero = jnp.zeros((8, 128), jnp.float32)
            total = [[(zero, zero)] * 3 for _ in range(4)]
            ahead = unflat(sh.along_x(flat(project(f, 0, -par)), True), 2)
            lift_add(total, link_times(link, 0, ahead, False), 0, -par)
            behind = flat(link_times(link, 0, project(f, 0, par), True))
            lift_add(total, unflat(sh.along_x(behind, False), 2), 0, par)
            for i, v in enumerate(flat(total)):
                acc[p, i] = v
            return _
        lax.fori_loop(first, end, body, 0)

    def receive_body(src, w, p, par):
        await_edges(w, p)
        await_time(w, p)
        f = load_field(src, p)
        total = load_field(acc, p)
        for kind, mu in ((0, 1), (1, 2)):
            got = [edge_in[w, 2 * kind, p, i] for i in range(3)]
            ahead = unflat(sh.shift(flat(project(f, mu, -par)), got, kind, True), 2)
            lift_add(total, link_times(link, mu, ahead, False), mu, -par)
            got = [edge_in[w, 2 * kind + 1, p, i] for i in range(3)]
            local = [carried[kind, p, i] for i in range(12)]
            lift_add(total, unflat(sh.shift(local, got, kind, False), 2), mu, par)
        ahead = unflat([time_in[w, 0, p, i] for i in range(12)], 2)
        lift_add(total, link_times(link, 3, ahead, False), 3, -par)
        lift_add(total, unflat([time_in[w, 1, p, i] for i in range(12)], 2), 3, par)
        return [a - HOP * b for a, b in zip(flat(f), flat(total))]

    def block_copy(slot, gz, device, to):
        return pltpu.make_async_remote_copy(
            src_ref=blocks.at[slot * n_gz + gz], dst_ref=blocks.at[to * n_gz + gz],
            send_sem=send_sem.at[2], recv_sem=block_sem.at[to * n_gz + gz],
            device_id=device, device_id_type=MESH,
        )

    mate = 1 - 2 * lax.rem(me["gz"], 2)
    direct = [(slot, z) for z in range(0, n_gz, 2) for slot in range(reach) if (slot, z) != (own, 0)]

    def send_blocks():
        block_copy(own, me["gz"], across(0, mate), own).start()
        for slot, z in direct:
            block_copy(own, me["gz"], across(own - slot, z), slot).start()

    def pass_blocks():
        for slot, z in direct:
            copy = block_copy(slot, lax.rem(me["gz"] - z + n_gz, n_gz), across(0, mate), slot)
            copy.wait_recv()
            copy.start()

    def await_blocks():
        for z in range(0, n_gz, 2):
            for slot in range(reach):
                block_copy(slot, lax.rem(me["gz"] + mate - z + 2 * n_gz, n_gz), across(0, mate), slot).wait_recv()

    def smt_copy(d):
        return pltpu.make_async_remote_copy(
            src_ref=smt_out.at[d], dst_ref=smt_in.at[d],
            send_sem=send_sem.at[3], recv_sem=smt_sem.at[0],
            device_id=peer("ta", 1 if isinstance(d, slice) else 2 * d - 1), device_id_type=MESH,
        )

    def widen(z, _):
        for g in range(groups):
            for i in range(55):
                wide[g, z, i, 0:4] = blocks[2 * g * n_gz + z, i]
                wide[g, z, i, 4:8] = blocks[(2 * g + 1) * n_gz + z, i]
        return _

    def links_of(g, z):
        return wide.at[g, z, pl.ds(1, 54)]

    def colour(ref, now, g, z, c):
        return [ref[now, g, z, c * 6 + i] for i in range(6)]

    def carry_hops(now, g, z):
        for c in range(3):
            vector = unflat(colour(smear, now, g, z, c), 1)
            for mu in (2,) if groups == 1 else (2, 1):
                for i, v in enumerate(flat(link_times(links_of(g, z), mu, vector, True))):
                    carry[2 - mu, now, g, z, c * 6 + i] = v

    def beyond(items, others, kind, ahead):
        outs = []
        for v, other in zip(items, others):
            step = -1 if ahead else 1
            inner = (sh.row if kind == 0 else sh.lane // LX)
            last = inner == ((7, 3)[kind] if ahead else 0)
            moved = sh.roll(v, kind, step)
            outs.append(moved if other is None else jnp.where(last, sh.roll(other, kind, step), moved))
        return outs

    def colour_hops(now, g, z, c):
        link_at = links_of(g, z)
        items = colour(smear, now, g, z, c)
        vector = unflat(items, 1)
        out = [(
            flat(link_times(link_at, 0, unflat(sh.along_x(items, True), 1), False)),
            sh.along_x(flat(link_times(link_at, 0, vector, True)), False),
        )]
        if groups == 1:
            later, behind, before = [None] * 6, flat(link_times(link_at, 1, vector, True)), [None] * 6
        else:
            later = colour(smear, now, (g + 1) % groups, z, c)
            behind = colour(carry.at[1], now, g, z, c)
            before = colour(carry.at[1], now, (g - 1) % groups, z, c)
        out.append((
            flat(link_times(link_at, 1, unflat(beyond(items, later, 0, True), 1), False)),
            beyond(behind, before, 0, False),
        ))
        later = colour(smear, now, g, lax.rem(z + 1, n_gz), c)
        behind = colour(carry.at[0], now, g, z, c)
        before = colour(carry.at[0], now, g, lax.rem(z + n_gz - 1, n_gz), c)
        out.append((
            flat(link_times(link_at, 2, unflat(beyond(items, later, 1, True), 1), False)),
            beyond(behind, before, 1, False),
        ))
        return items, out

    def from_points(g, z):
        point = wide[g, z, 0]
        return [
            [[(wide[g, z, 1 + mu * 18 + c * 3 + a] * point, wide[g, z, 10 + mu * 18 + c * 3 + a] * -point)
              for a in range(3)] for c in range(3)]
            for mu in range(3)
        ]

    def first_step(k, _):
        z = lax.rem(me["gz"] + k, n_gz)
        for g in range(groups):
            point = wide[g, z, 0]
            after, before = lax.rem(z + 1, n_gz), lax.rem(z + n_gz - 1, n_gz)
            up = None if groups == 1 else wide[(g + 1) % groups, z, 0]
            ahead = [
                sh.along_x([point], True)[0], beyond([point], [up], 0, True)[0],
                beyond([point], [wide[g, after, 0]], 1, True)[0],
            ]
            back = from_points(g, z)
            below = None if groups == 1 else from_points((g - 1) % groups, z)
            beside = from_points(g, before)
            for c in range(3):
                sides = [
                    sh.along_x(flat([back[0][c]]), False),
                    beyond(flat([back[1][c]]), [None] * 6 if groups == 1 else flat([below[1][c]]), 0, False),
                    beyond(flat([back[2][c]]), flat([beside[2][c]]), 1, False),
                ]
                for part in range(2):
                    for a in range(3):
                        i = part * 3 + a
                        total = None
                        for mu in range(3):
                            term = wide[g, z, 1 + mu * 18 + part * 9 + a * 3 + c] * ahead[mu] + sides[mu][i]
                            total = term if total is None else total + term
                        value = 0.25 * total if i != c else point + 0.25 * total
                        smear[1, g, z, c * 6 + i] = value * 0.5
            carry_hops(1, g, z)
        return _

    def smear_steps(first, end):
        for step in range(first, end):
            now, then = step % 2, (step + 1) % 2
            deep = min(-(-(NSMEAR - step) // (128 // LX)), n_gz // 2)

            def body(k, _):
                z = lax.rem(me["gz"] - deep + k + n_gz, n_gz)
                for g in range(groups):
                    for c in range(3):
                        items, parts = colour_hops(now, g, z, c)
                        for i, v in enumerate(items):
                            total = None
                            for ahead, behind in parts:
                                part = ahead[i] + behind[i]
                                total = part if total is None else total + part
                            smear[then, g, z, c * 6 + i] = (v + 0.25 * total) * 0.5
                    carry_hops(then, g, z)
                return _

            lax.fori_loop(0, min(2 * deep + 1, n_gz), body, 0)

    def both_halves(items):
        return [jnp.where(sh.low, v, pltpu.roll(v, 4, 0)) for v in items]

    def start_right(items):
        carried_on = flat(link_times(link, 3, unflat(items, 1), True))
        for d, values in enumerate((items, carried_on)):
            for a in range(3):
                smt_out[d, a] = jnp.where(sh.low, values[a], values[3 + a])
            smt_copy(d).start()

    def from_time(d):
        got = [smt_in[d, a] for a in range(3)]
        turned = [pltpu.roll(v, 4, 0) for v in got]
        real = [jnp.where(sh.low, v, t) for v, t in zip(got, turned)]
        return real + [jnp.where(sh.low, t, v) for v, t in zip(got, turned)]

    def take(mu, items, ahead, behind):
        for i in range(6):
            hops[mu, i] = HOP * (behind[i] - ahead[i])
            part = HOP * (ahead[i] + behind[i])
            hops[4, i] = items[i] - part if mu == 0 else hops[4, i] - part

    def local_right(items):
        parts = colour_hops(NSMEAR % 2, own // 2, me["gz"], 0)[1]
        for mu in range(3):
            take(mu, items, *(both_halves(side) for side in parts[mu]))

    def finish_right():
        smt_copy(slice(None)).wait_recv()
        take(3, None, flat(link_times(link, 3, unflat(from_time(0), 1), False)), from_time(1))
        zero = jnp.zeros((8, 128), jnp.float32)

        def pick(which, a):
            return hops[which, a], hops[which, 3 + a]

        def block(s2, s, a):
            if s2 == s:
                return pick(4, a)
            if s2 // 2 == s // 2:
                return (zero, zero)
            out = (zero, zero)
            for mu in range(4):
                for row in range(2):
                    column, coef = E_ROWS[mu][row]
                    if s2 < 2 and row == s2 and column == s - 2:
                        out = add_term(out, coef, pick(mu, a))
                    if s2 >= 2 and column == s2 - 2 and row == s:
                        out = add_term(out, complex(coef).conjugate(), pick(mu, a))
            return out

        for h in range(2):
            for s2 in range(4):
                for a in range(3):
                    up, down = (block(s2, 2 * h + k, a) for k in range(2))
                    for part in range(2):
                        right[h, part * 12 + s2 * 3 + a] = jnp.where(sh.low, up[part], down[part])

    def first_time(p, _):
        load_guess(p, 0)
        send_time(load_field(guess, p), 0, p, 1)
        return _

    def first_edges(p, _):
        send_edges(load_field(guess, p), 0, p, 1)
        return _

    def give(ref, p, out):
        first, second_rhs = rhs_of(p)
        for i, v in enumerate(out):
            place = pl.ds(4 * (i % 2), 4)
            ref[first, i // 2, place] = v[0:4]
            ref[second_rhs, i // 2, place] = v[4:8]

    def second(p, _):
        out = receive_body(guess, 0, p, 1)
        for i, v in enumerate(out):
            field_a[p, i] = v
        send_time(unflat(out, 4), 1, p, -1)
        send_edges(unflat(out, 4), 1, p, -1)
        return _

    def second_late(p, _):
        spin = 2 * lax.rem(p, 2) + jnp.where(sh.low, 0, 1)
        out = receive_body(guess, 0, p, 1)
        for part in range(2):
            for s2 in range(4):
                for a in range(3):
                    i = part * 12 + s2 * 3 + a
                    source = jnp.where(spin == s2, sources[p // 2, part * 3 + a], 0.0)
                    out[i] = out[i] - source
        for i, v in enumerate(out):
            field_a[p, i] = v
        send_time(unflat(out, 4), 1, p, -1)
        send_edges(unflat(out, 4), 1, p, -1)
        return _

    def no_right(p, _):
        for i in range(24):
            right[p, i] = jnp.zeros((8, 128), jnp.float32)
        return _

    def third(p, _):
        out = [right[p, i] - v for i, v in enumerate(receive_body(field_a, 1, p, -1))]
        total = None
        for i, v in enumerate(out):
            search[p, i] = v
            total = v * v if total is None else total + v * v
        sums[p] = total
        give(search_ref, p, out)
        send_time(unflat(out, 4), 2, p, 1)
        send_edges(unflat(out, 4), 2, p, 1)
        return _

    def run(body, first, end):
        lax.fori_loop(first, end, body, 0)

    send_blocks()
    run(first_time, 0, PAIRS)
    double_links(0, 54)
    run(first_edges, 0, PAIRS)
    interior(guess, 1)
    pass_blocks()
    run(second, 0, 1)
    await_blocks()
    lax.fori_loop(0, n_gz, widen, 0)
    lax.fori_loop(0, n_gz, first_step, 0)
    smear_steps(1, 3)
    run(second, 1, 2)
    smear_steps(3, NSMEAR)
    for c in range(3):
        for i, v in enumerate(both_halves(colour(smear, NSMEAR % 2, own // 2, me["gz"], c))):
            sources[c, i] = v
    items = [sources[0, i] for i in range(6)]
    start_right(items)
    run(second_late, 2, PAIRS)
    local_right(items)
    interior(field_a, -1)
    run(no_right, 2, PAIRS)
    finish_right()

    run(third, 0, PAIRS)
    interior(search, 1)

    def fourth(p, _):
        out = receive_body(search, 2, p, 1)
        total = None
        for i, v in enumerate(out):
            field_b[p, i] = v
            total = v * v if total is None else total + v * v
        sums[PAIRS + p] = total
        send_time(unflat(out, 4), 3, p, -1, held=True)
        send_edges(unflat(out, 4), 3, p, -1)
        return _

    run(fourth, 0, PAIRS)

    def normal_of(p, _):
        give(normal_ref, p, receive_body(field_b, 3, p, -1))
        return _

    mine = jnp.zeros((8, 128), jnp.float32)
    for k in range(2 * PAIRS):
        mine = jnp.where(sh.lane == k, jnp.sum(sums[k], axis=1, keepdims=True), mine)
    slot = 0
    for stage, axis in enumerate(AXES):
        red_out[stage] = mine
        others = n_of[axis] - 1

        def sum_copy(k, place):
            return pltpu.make_async_remote_copy(
                src_ref=red_out.at[stage], dst_ref=red_in.at[place],
                send_sem=send_sem.at[4], recv_sem=red_sem.at[stage],
                device_id=peer(axis, k), device_id_type=MESH,
            )

        for k in range(1, others + 1):
            sum_copy(k, slot + k - 1).start()
        if stage == 0:
            interior(field_b, -1)
        if stage == 2:
            pl.when(first_core)(lambda: start_time(3, PAIRS - 1))
            run(normal_of, 0, PAIRS - 3)
            pl.when(other_core)(lambda: start_time(3, PAIRS - 2))
            run(normal_of, PAIRS - 3, PAIRS - 2)
            pl.when(other_core)(lambda: start_time(3, PAIRS - 1))
            run(normal_of, PAIRS - 2, PAIRS - 1)
        landed = red_in.at[pl.ds(slot, others)]
        pltpu.make_async_remote_copy(
            src_ref=landed, dst_ref=landed, send_sem=send_sem.at[4], recv_sem=red_sem.at[stage],
            device_id=peer(axis, 1), device_id_type=MESH,
        ).wait_recv()
        for k in range(others):
            mine = mine + red_in[slot + k]
        slot += others
    top = jnp.sum(mine[0:4], axis=0, keepdims=True)
    bottom = jnp.sum(mine[4:8], axis=0, keepdims=True)
    both = jnp.where(sh.low, top, bottom)
    curvature = pltpu.roll(both, 128 - PAIRS, 1)
    steps = both / jnp.where(sh.lane < PAIRS, curvature, 1.0)

    for p in range(PAIRS):
        length = jnp.sum(jnp.where(sh.lane == p, steps, 0.0), axis=1, keepdims=True)
        first = 6 * (p % 2) + p // 2
        second_rhs = first + 3
        length_ref[first : first + 1] = jnp.broadcast_to(length[0:1], (1, 128))
        length_ref[second_rhs : second_rhs + 1] = jnp.broadcast_to(length[4:5], (1, 128))

    run(normal_of, PAIRS - 1, PAIRS)

    passed = blocks.at[pl.ds(0, reach * n_gz - 1)]
    for k, (sent, landed) in enumerate((
        (edge_out, edge_in), (time_out, time_in), (passed, passed), (smt_out, smt_in), (red_in, red_in),
    )):
        pltpu.make_async_remote_copy(
            src_ref=sent, dst_ref=landed, send_sem=send_sem.at[k], recv_sem=red_sem.at[0],
            device_id=peer("ta", 1), device_id_type=MESH,
        ).wait_send()


def on_device(sizes, links, guess, source_sites):
    rows, lanes = guess.shape[-2:]
    f32 = jnp.float32
    copies = sum(n - 1 for n in sizes)
    n_gz = sizes[AXES.index("gz")]
    reach = min(sizes[0], 8)
    groups = reach // 2
    tile = (8, lanes)
    vm = lambda *shape: pltpu.VMEM(shape + tile, f32)
    dma = lambda *shape: pltpu.SemaphoreType.DMA(shape)
    out = jax.ShapeDtypeStruct((12, 12, 2 * rows, lanes), f32)
    search, normal, length = pl.pallas_call(
        functools.partial(kernel, sizes),
        out_shape=(out, out, jax.ShapeDtypeStruct((12, lanes), f32)),
        in_specs=[
            pl.BlockSpec(memory_space=pltpu.HBM),
            pl.BlockSpec(memory_space=pltpu.HBM),
            pl.BlockSpec(memory_space=pltpu.HBM),
        ],
        out_specs=(pl.BlockSpec(memory_space=pltpu.VMEM),) * 3,
        scratch_shapes=[
            pltpu.SMEM((4,), jnp.int32), pltpu.VMEM((72, rows, lanes), f32), pltpu.VMEM((12, 24, rows, lanes), f32),
            pltpu.VMEM((reach * n_gz, 55, rows, lanes), f32), vm(groups, n_gz, 55),
            vm(2, groups, n_gz, 18), vm(min(groups, 2), 2, groups, n_gz, 18),
            vm(72), vm(PAIRS, 24), vm(PAIRS, 24), vm(PAIRS, 24), vm(PAIRS, 24), vm(PAIRS, 24),
            vm(PAIRS, 24), vm(2, PAIRS, 12),
            vm(4, 4, PAIRS, 3), vm(4, 4, PAIRS, 3), vm(4, 2, PAIRS, 12), vm(4, 2, PAIRS, 12),
            vm(2, 3), vm(2, 3),
            vm(3), vm(copies), vm(2 * PAIRS), vm(5, 6), vm(3, 6),
            dma(4), dma(2, PAIRS // EDGE_CHUNK), dma(2, PAIRS), dma(reach * n_gz), dma(1), dma(3), dma(5),
        ],
        compiler_params=pltpu.CompilerParams(
            collective_id=0, has_side_effects=True, vmem_limit_bytes=48 * 1024 * 1024
        ),
    )(*(
        pltpu.with_memory_space_constraint(x, pltpu.HBM)
        for x in (
            source_sites.reshape(4), links.reshape(72, rows, lanes), guess.reshape(12, 24, rows, lanes)
        )
    ))
    length = length[:, None, None]
    sol = guess.reshape(search.shape) + length * search
    res = search - length * normal
    return sol.reshape(guess.shape), res.reshape(guess.shape)


def solution(mesh):
    sizes = tuple(mesh.shape[axis] for axis in AXES)
    fields = P(None, None, None, None, "ta", "xy", "gz")
    return jax.shard_map(
        functools.partial(on_device, sizes),
        mesh=mesh,
        in_specs=(fields, fields, P("ta", "xy", "gz", None)),
        out_specs=(fields, fields),
        check_vma=False,
    )
```

```python
import functools

import jax
import jax.numpy as jnp
from jax import lax
from jax.experimental import pallas as pl
from jax.experimental.pallas import tpu as pltpu
from jax.sharding import PartitionSpec as P

LX = 32
NSMEAR = 8
HOP = 0.12
PAIRS = 6
EDGE_CHUNK = 3
TIME_CHUNK = 1
MESH = pl.DeviceIdType.MESH
AXES = ("xy", "gz", "ta")

E_ROWS = (
    ((1, -1j), (0, -1j)),
    ((1, -1), (0, 1)),
    ((0, -1j), (1, 1j)),
    ((0, 1), (1, 1)),
)


def times(coef, z):
    re, im = z
    if coef == 1:
        return (1, re), (1, im)
    if coef == -1:
        return (-1, re), (-1, im)
    if coef == 1j:
        return (-1, im), (1, re)
    return (1, im), (-1, re)


def add_term(z, coef, other):
    out = []
    for base, (sign, term) in zip(z, times(coef, other)):
        out.append(base + term if sign > 0 else base - term)
    return tuple(out)


def project(f, mu, parity):
    half = []
    for row in range(2):
        column, coef = E_ROWS[mu][row]
        half.append([add_term(f[row][a], parity * coef, f[2 + column][a]) for a in range(3)])
    return half


def lift_add(total, h, mu, parity):
    for row in range(2):
        column, coef = E_ROWS[mu][row]
        for a in range(3):
            total[row][a] = add_term(total[row][a], 1, h[row][a])
            low = parity * complex(coef).conjugate()
            total[2 + column][a] = add_term(total[2 + column][a], low, h[row][a])


def link_times(link, mu, vectors, adjoint):
    def entry(a, b):
        if adjoint:
            a, b = b, a
        base = mu * 18 + a * 3 + b
        return link[base], link[base + 9]

    out = [[None] * 3 for _ in vectors]
    for a in range(3):
        totals = [None] * len(vectors)
        for b in range(3):
            ur, ui = entry(a, b)
            for k, vec in enumerate(vectors):
                re, im = vec[b]
                if adjoint:
                    tr, ti = ur * re + ui * im, ur * im - ui * re
                else:
                    tr, ti = ur * re - ui * im, ur * im + ui * re
                old = totals[k]
                totals[k] = (tr, ti) if old is None else (old[0] + tr, old[1] + ti)
        for k in range(len(vectors)):
            out[k][a] = totals[k]
    return out


def flat(vectors):
    return [vec[a][part] for part in range(2) for vec in vectors for a in range(3)]


def unflat(items, count):
    return [
        [(items[k * 3 + a], items[3 * count + k * 3 + a]) for a in range(3)] for k in range(count)
    ]


class Shifts:
    def __init__(self):
        row = lax.broadcasted_iota(jnp.int32, (8, 128), 0)
        lane = lax.broadcasted_iota(jnp.int32, (8, 128), 1)
        self.low = row < 4
        self.row = row
        self.lane = lane
        self.place = ([row % 4 == k for k in range(4)], [lane // LX == k for k in range(4)])
        self.x_first = lane % LX == 0
        self.x_last = lane % LX == LX - 1
        self.unit = ((0, 1, 8), (1, LX, 128))

    def roll(self, v, kind, steps):
        axis, unit, size = self.unit[kind]
        amount = (steps * unit) % size
        return v if amount == 0 else pltpu.roll(v, amount, axis)

    def pack(self, items, kind, ahead):
        packed = []
        for g in range(0, len(items), 4):
            out = None
            for k in range(4):
                v = self.roll(items[g + k], kind, k if ahead else k - 3)
                out = v if out is None else jnp.where(self.place[kind][k], v, out)
            packed.append(out)
        return packed

    def shift(self, items, packed, kind, ahead):
        outs = []
        for i, v in enumerate(items):
            got = packed[i // 4]
            k = i % 4
            if ahead:
                moved = self.roll(v, kind, -1)
                outs.append(jnp.where(self.place[kind][3], self.roll(got, kind, 3 - k), moved))
            else:
                moved = self.roll(v, kind, 1)
                outs.append(jnp.where(self.place[kind][0], self.roll(got, kind, -k), moved))
        return outs

    def along_x(self, items, ahead):
        outs = []
        for v in items:
            if ahead:
                a, b = pltpu.roll(v, 127, 1), pltpu.roll(v, LX - 1, 1)
                outs.append(jnp.where(self.x_last, b, a))
            else:
                a, b = pltpu.roll(v, 1, 1), pltpu.roll(v, 129 - LX, 1)
                outs.append(jnp.where(self.x_first, b, a))
        return outs


def kernel(
    sizes, sites_hbm, links_hbm, guess_hbm, search_ref, normal_ref, length_ref,
    sites_ref, links_ref, guess_ref, blocks, wide, smear, carry,
    link, guess, field_a, field_b, search, acc, right, carried,
    edge_out, edge_in, time_out, time_in, smt_out, smt_in,
    red_out, red_in, sums, hops, sources,
    load_sem, edge_sem, time_sem, block_sem, smt_sem, red_sem, send_sem,
):
    n_of = dict(zip(AXES, sizes))
    me = {axis: lax.axis_index(axis) for axis in AXES}
    n_gz = n_of["gz"]
    reach = min(n_of["xy"], 8)
    own = 0 if reach == n_of["xy"] else reach // 2
    groups = reach // 2

    loads = [
        pltpu.make_async_copy(src, dst, load_sem.at[k])
        for k, (src, dst) in enumerate((
            (links_hbm, links_ref), (sites_hbm, sites_ref), (guess_hbm, guess_ref),
            (links_hbm.at[pl.ds(0, 54)], blocks.at[own * n_gz + me["gz"], pl.ds(1, 54)]),
        ))
    ]
    for k in (3, 1, 0, 2):
        loads[k].start()

    def peer(axis, step):
        return {axis: lax.rem(me[axis] + step + n_of[axis], n_of[axis])}

    def across(xy, gz):
        return {
            "xy": lax.rem(me["xy"] + xy + n_of["xy"], n_of["xy"]),
            "gz": lax.rem(me["gz"] + gz + n_gz, n_gz),
        }

    shifts = sorted({(slot - own) % n_of["xy"] for slot in range(reach)} | {(own - slot) % n_of["xy"] for slot in range(reach)})
    greeted = [across(y, z) for y in shifts for z in range(0, n_gz, 1 if y == 0 else 2) if (y, z) != (0, 0)]
    greeted += [peer("xy", y) for y in range(1, n_of["xy"]) if y not in shifts]
    greeted += [peer("ta", t) for t in range(1, n_of["ta"])]
    barrier = pltpu.get_barrier_semaphore()
    for device in greeted:
        pl.semaphore_signal(barrier, inc=1, device_id=device, device_id_type=MESH)

    sh = Shifts()

    row = lax.broadcasted_iota(jnp.int32, (4, 128), 0)
    lane = lax.broadcasted_iota(jnp.int32, (4, 128), 1)
    loads[3].wait()
    loads[1].wait()
    hit = (row == sites_ref[1]) & (lane == sites_ref[2] * LX + sites_ref[3])
    hit = hit & (sites_ref[0] == 0)
    blocks[own * n_gz + me["gz"], 0] = jnp.where(hit, 1.0, 0.0).astype(jnp.float32)

    loads[0].wait()
    sign = jnp.where(me["ta"] == n_of["ta"] - 1, -1.0, 1.0).astype(jnp.float32)

    def double_links(first, end):
        for i in range(first, end):
            v = links_ref[i]
            if i >= 54:
                v = v * sign
            link[i, 0:4, :] = v
            link[i, 4:8, :] = v

    double_links(54, 72)

    def rhs_of(p):
        first = 6 * lax.rem(p, 2) + p // 2
        return first, first + 3

    def load_guess(p, _):
        first, second = rhs_of(p)
        for i in range(24):
            guess[p, i, 0:4, :] = guess_ref[first, i]
            guess[p, i, 4:8, :] = guess_ref[second, i]
        return _

    loads[2].wait()
    pl.semaphore_wait(barrier, len(greeted))

    def part_of(p, chunk):
        return pl.ds(p, chunk)

    def start_last(make, w, d, p, chunk):
        if chunk == 1:
            make(w, d, p).start()
        else:
            @pl.when(lax.rem(p, chunk) == chunk - 1)
            def _():
                make(w, d, p - (chunk - 1)).start()

    def edge_copy(w, d, p):
        axis, step = (("xy", -1), ("xy", 1), ("gz", -1), ("gz", 1))[0 if isinstance(d, slice) else d]
        return pltpu.make_async_remote_copy(
            src_ref=edge_out.at[w, d, part_of(p, EDGE_CHUNK)], dst_ref=edge_in.at[w, d, part_of(p, EDGE_CHUNK)],
            send_sem=send_sem.at[0], recv_sem=edge_sem.at[lax.rem(w, 2), p // EDGE_CHUNK],
            device_id=peer(axis, step), device_id_type=MESH,
        )

    def time_copy(w, d, p):
        return pltpu.make_async_remote_copy(
            src_ref=time_out.at[w, d, part_of(p, TIME_CHUNK)], dst_ref=time_in.at[w, d, part_of(p, TIME_CHUNK)],
            send_sem=send_sem.at[1], recv_sem=time_sem.at[lax.rem(w, 2), p],
            device_id=peer("ta", 1 if isinstance(d, slice) else 2 * d - 1), device_id_type=MESH,
        )

    def await_edges(w, p):
        def wait():
            edge_copy(w, slice(None), p).wait_recv()

        pl.when(lax.rem(p, EDGE_CHUNK) == 0)(wait)

    def await_time(w, p):
        time_copy(w, slice(None), p).wait_recv()

    def load_field(ref, p):
        return unflat([ref[p, i] for i in range(24)], 4)

    first_core = lax.rem(me["gz"], 2) == 0
    other_core = lax.rem(me["gz"], 2) == 1

    def send_time(f, w, p, par, held=False):
        for i, v in enumerate(flat(project(f, 3, -par))):
            time_out[w, 0, p, i] = v
        for i, v in enumerate(flat(link_times(link, 3, project(f, 3, par), True))):
            time_out[w, 1, p, i] = v
        if held:
            pl.when((p < PAIRS - 2) | ((p < PAIRS - 1) & first_core))(lambda: start_time(w, p))
        else:
            start_time(w, p)

    def start_time(w, p):
        last = jnp.where(me["ta"] == n_of["ta"] - 1, 1, 0)
        for d in (last, 1 - last):
            time_copy(w, d, p).start()

    def send_edges(f, w, p, par):
        for kind, mu in ((0, 1), (1, 2)):
            for i, v in enumerate(sh.pack(flat(project(f, mu, -par)), kind, True)):
                edge_out[w, 2 * kind, p, i] = v
            start_last(edge_copy, w, 2 * kind, p, EDGE_CHUNK)
            behind = flat(link_times(link, mu, project(f, mu, par), True))
            for i, v in enumerate(behind):
                carried[kind, p, i] = v
            for i, v in enumerate(sh.pack(behind, kind, False)):
                edge_out[w, 2 * kind + 1, p, i] = v
            start_last(edge_copy, w, 2 * kind + 1, p, EDGE_CHUNK)

    def interior(src, par, first=0, end=PAIRS):
        def body(p, _):
            f = load_field(src, p)
            zero = jnp.zeros((8, 128), jnp.float32)
            total = [[(zero, zero)] * 3 for _ in range(4)]
            ahead = unflat(sh.along_x(flat(project(f, 0, -par)), True), 2)
            lift_add(total, link_times(link, 0, ahead, False), 0, -par)
            behind = flat(link_times(link, 0, project(f, 0, par), True))
            lift_add(total, unflat(sh.along_x(behind, False), 2), 0, par)
            for i, v in enumerate(flat(total)):
                acc[p, i] = v
            return _
        lax.fori_loop(first, end, body, 0)

    def receive_body(src, w, p, par):
        await_edges(w, p)
        await_time(w, p)
        f = load_field(src, p)
        total = load_field(acc, p)
        for kind, mu in ((0, 1), (1, 2)):
            got = [edge_in[w, 2 * kind, p, i] for i in range(3)]
            ahead = unflat(sh.shift(flat(project(f, mu, -par)), got, kind, True), 2)
            lift_add(total, link_times(link, mu, ahead, False), mu, -par)
            got = [edge_in[w, 2 * kind + 1, p, i] for i in range(3)]
            local = [carried[kind, p, i] for i in range(12)]
            lift_add(total, unflat(sh.shift(local, got, kind, False), 2), mu, par)
        ahead = unflat([time_in[w, 0, p, i] for i in range(12)], 2)
        lift_add(total, link_times(link, 3, ahead, False), 3, -par)
        lift_add(total, unflat([time_in[w, 1, p, i] for i in range(12)], 2), 3, par)
        return [a - HOP * b for a, b in zip(flat(f), flat(total))]

    def block_copy(slot, gz, device, to):
        return pltpu.make_async_remote_copy(
            src_ref=blocks.at[slot * n_gz + gz], dst_ref=blocks.at[to * n_gz + gz],
            send_sem=send_sem.at[2], recv_sem=block_sem.at[to * n_gz + gz],
            device_id=device, device_id_type=MESH,
        )

    mate = 1 - 2 * lax.rem(me["gz"], 2)
    direct = [(slot, z) for z in range(0, n_gz, 2) for slot in range(reach) if (slot, z) != (own, 0)]

    def send_blocks():
        block_copy(own, me["gz"], across(0, mate), own).start()
        for slot, z in direct:
            block_copy(own, me["gz"], across(own - slot, z), slot).start()

    def pass_blocks():
        for slot, z in direct:
            copy = block_copy(slot, lax.rem(me["gz"] - z + n_gz, n_gz), across(0, mate), slot)
            copy.wait_recv()
            copy.start()

    def await_blocks():
        for z in range(0, n_gz, 2):
            for slot in range(reach):
                block_copy(slot, lax.rem(me["gz"] + mate - z + 2 * n_gz, n_gz), across(0, mate), slot).wait_recv()

    def smt_copy(d):
        return pltpu.make_async_remote_copy(
            src_ref=smt_out.at[d], dst_ref=smt_in.at[d],
            send_sem=send_sem.at[3], recv_sem=smt_sem.at[0],
            device_id=peer("ta", 1 if isinstance(d, slice) else 2 * d - 1), device_id_type=MESH,
        )

    def widen(z, _):
        for g in range(groups):
            for i in range(55):
                wide[g, z, i, 0:4] = blocks[2 * g * n_gz + z, i]
                wide[g, z, i, 4:8] = blocks[(2 * g + 1) * n_gz + z, i]
        return _

    def links_of(g, z):
        return wide.at[g, z, pl.ds(1, 54)]

    def colour(ref, now, g, z, c):
        return [ref[now, g, z, c * 6 + i] for i in range(6)]

    def carry_hops(now, g, z):
        for c in range(3):
            vector = unflat(colour(smear, now, g, z, c), 1)
            for mu in (2,) if groups == 1 else (2, 1):
                for i, v in enumerate(flat(link_times(links_of(g, z), mu, vector, True))):
                    carry[2 - mu, now, g, z, c * 6 + i] = v

    def beyond(items, others, kind, ahead):
        outs = []
        for v, other in zip(items, others):
            step = -1 if ahead else 1
            inner = (sh.row if kind == 0 else sh.lane // LX)
            last = inner == ((7, 3)[kind] if ahead else 0)
            moved = sh.roll(v, kind, step)
            outs.append(moved if other is None else jnp.where(last, sh.roll(other, kind, step), moved))
        return outs

    def colour_hops(now, g, z, c):
        link_at = links_of(g, z)
        items = colour(smear, now, g, z, c)
        vector = unflat(items, 1)
        out = [(
            flat(link_times(link_at, 0, unflat(sh.along_x(items, True), 1), False)),
            sh.along_x(flat(link_times(link_at, 0, vector, True)), False),
        )]
        if groups == 1:
            later, behind, before = [None] * 6, flat(link_times(link_at, 1, vector, True)), [None] * 6
        else:
            later = colour(smear, now, (g + 1) % groups, z, c)
            behind = colour(carry.at[1], now, g, z, c)
            before = colour(carry.at[1], now, (g - 1) % groups, z, c)
        out.append((
            flat(link_times(link_at, 1, unflat(beyond(items, later, 0, True), 1), False)),
            beyond(behind, before, 0, False),
        ))
        later = colour(smear, now, g, lax.rem(z + 1, n_gz), c)
        behind = colour(carry.at[0], now, g, z, c)
        before = colour(carry.at[0], now, g, lax.rem(z + n_gz - 1, n_gz), c)
        out.append((
            flat(link_times(link_at, 2, unflat(beyond(items, later, 1, True), 1), False)),
            beyond(behind, before, 1, False),
        ))
        return items, out

    def from_points(g, z):
        point = wide[g, z, 0]
        return [
            [[(wide[g, z, 1 + mu * 18 + c * 3 + a] * point, wide[g, z, 10 + mu * 18 + c * 3 + a] * -point)
              for a in range(3)] for c in range(3)]
            for mu in range(3)
        ]

    def first_step(k, _):
        z = lax.rem(me["gz"] + k, n_gz)
        for g in range(groups):
            point = wide[g, z, 0]
            after, before = lax.rem(z + 1, n_gz), lax.rem(z + n_gz - 1, n_gz)
            up = None if groups == 1 else wide[(g + 1) % groups, z, 0]
            ahead = [
                sh.along_x([point], True)[0], beyond([point], [up], 0, True)[0],
                beyond([point], [wide[g, after, 0]], 1, True)[0],
            ]
            back = from_points(g, z)
            below = None if groups == 1 else from_points((g - 1) % groups, z)
            beside = from_points(g, before)
            for c in range(3):
                sides = [
                    sh.along_x(flat([back[0][c]]), False),
                    beyond(flat([back[1][c]]), [None] * 6 if groups == 1 else flat([below[1][c]]), 0, False),
                    beyond(flat([back[2][c]]), flat([beside[2][c]]), 1, False),
                ]
                for part in range(2):
                    for a in range(3):
                        i = part * 3 + a
                        total = None
                        for mu in range(3):
                            term = wide[g, z, 1 + mu * 18 + part * 9 + a * 3 + c] * ahead[mu] + sides[mu][i]
                            total = term if total is None else total + term
                        value = 0.25 * total if i != c else point + 0.25 * total
                        smear[1, g, z, c * 6 + i] = value * 0.5
            carry_hops(1, g, z)
        return _

    def smear_steps(first, end):
        for step in range(first, end):
            now, then = step % 2, (step + 1) % 2
            deep = min(-(-(NSMEAR - step) // (128 // LX)), n_gz // 2)

            def body(k, _):
                z = lax.rem(me["gz"] - deep + k + n_gz, n_gz)
                for g in range(groups):
                    for c in range(3):
                        items, parts = colour_hops(now, g, z, c)
                        for i, v in enumerate(items):
                            total = None
                            for ahead, behind in parts:
                                part = ahead[i] + behind[i]
                                total = part if total is None else total + part
                            smear[then, g, z, c * 6 + i] = (v + 0.25 * total) * 0.5
                    carry_hops(then, g, z)
                return _

            lax.fori_loop(0, min(2 * deep + 1, n_gz), body, 0)

    def both_halves(items):
        return [jnp.where(sh.low, v, pltpu.roll(v, 4, 0)) for v in items]

    def start_right(items):
        carried_on = flat(link_times(link, 3, unflat(items, 1), True))
        for d, values in enumerate((items, carried_on)):
            for a in range(3):
                smt_out[d, a] = jnp.where(sh.low, values[a], values[3 + a])
            smt_copy(d).start()

    def from_time(d):
        got = [smt_in[d, a] for a in range(3)]
        turned = [pltpu.roll(v, 4, 0) for v in got]
        real = [jnp.where(sh.low, v, t) for v, t in zip(got, turned)]
        return real + [jnp.where(sh.low, t, v) for v, t in zip(got, turned)]

    def take(mu, items, ahead, behind):
        for i in range(6):
            hops[mu, i] = HOP * (behind[i] - ahead[i])
            part = HOP * (ahead[i] + behind[i])
            hops[4, i] = items[i] - part if mu == 0 else hops[4, i] - part

    def local_right(items):
        parts = colour_hops(NSMEAR % 2, own // 2, me["gz"], 0)[1]
        for mu in range(3):
            take(mu, items, *(both_halves(side) for side in parts[mu]))

    def finish_right():
        smt_copy(slice(None)).wait_recv()
        take(3, None, flat(link_times(link, 3, unflat(from_time(0), 1), False)), from_time(1))
        zero = jnp.zeros((8, 128), jnp.float32)

        def pick(which, a):
            return hops[which, a], hops[which, 3 + a]

        def block(s2, s, a):
            if s2 == s:
                return pick(4, a)
            if s2 // 2 == s // 2:
                return (zero, zero)
            out = (zero, zero)
            for mu in range(4):
                for row in range(2):
                    column, coef = E_ROWS[mu][row]
                    if s2 < 2 and row == s2 and column == s - 2:
                        out = add_term(out, coef, pick(mu, a))
                    if s2 >= 2 and column == s2 - 2 and row == s:
                        out = add_term(out, complex(coef).conjugate(), pick(mu, a))
            return out

        for h in range(2):
            for s2 in range(4):
                for a in range(3):
                    up, down = (block(s2, 2 * h + k, a) for k in range(2))
                    for part in range(2):
                        right[h, part * 12 + s2 * 3 + a] = jnp.where(sh.low, up[part], down[part])

    def first_time(p, _):
        load_guess(p, 0)
        send_time(load_field(guess, p), 0, p, 1)
        return _

    def first_edges(p, _):
        send_edges(load_field(guess, p), 0, p, 1)
        return _

    def give(ref, p, out):
        first, second_rhs = rhs_of(p)
        for i, v in enumerate(out):
            place = pl.ds(4 * (i % 2), 4)
            ref[first, i // 2, place] = v[0:4]
            ref[second_rhs, i // 2, place] = v[4:8]

    def second(p, _):
        out = receive_body(guess, 0, p, 1)
        for i, v in enumerate(out):
            field_a[p, i] = v
        send_time(unflat(out, 4), 1, p, -1)
        send_edges(unflat(out, 4), 1, p, -1)
        return _

    def second_late(p, _):
        spin = 2 * lax.rem(p, 2) + jnp.where(sh.low, 0, 1)
        out = receive_body(guess, 0, p, 1)
        for part in range(2):
            for s2 in range(4):
                for a in range(3):
                    i = part * 12 + s2 * 3 + a
                    source = jnp.where(spin == s2, sources[p // 2, part * 3 + a], 0.0)
                    out[i] = out[i] - source
        for i, v in enumerate(out):
            field_a[p, i] = v
        send_time(unflat(out, 4), 1, p, -1)
        send_edges(unflat(out, 4), 1, p, -1)
        return _

    def no_right(p, _):
        for i in range(24):
            right[p, i] = jnp.zeros((8, 128), jnp.float32)
        return _

    def third(p, _):
        out = [right[p, i] - v for i, v in enumerate(receive_body(field_a, 1, p, -1))]
        total = None
        for i, v in enumerate(out):
            search[p, i] = v
            total = v * v if total is None else total + v * v
        sums[p] = total
        give(search_ref, p, out)
        send_time(unflat(out, 4), 2, p, 1)
        send_edges(unflat(out, 4), 2, p, 1)
        return _

    def run(body, first, end):
        lax.fori_loop(first, end, body, 0)

    send_blocks()
    run(first_time, 0, PAIRS)
    double_links(0, 54)
    run(first_edges, 0, PAIRS)
    interior(guess, 1)
    pass_blocks()
    run(second, 0, 1)
    await_blocks()
    lax.fori_loop(0, n_gz, widen, 0)
    lax.fori_loop(0, n_gz, first_step, 0)
    smear_steps(1, 3)
    run(second, 1, 2)
    smear_steps(3, NSMEAR)
    for c in range(3):
        for i, v in enumerate(both_halves(colour(smear, NSMEAR % 2, own // 2, me["gz"], c))):
            sources[c, i] = v
    items = [sources[0, i] for i in range(6)]
    start_right(items)
    run(second_late, 2, PAIRS)
    local_right(items)
    interior(field_a, -1)
    run(no_right, 2, PAIRS)
    finish_right()

    run(third, 0, PAIRS)
    interior(search, 1)

    def fourth(p, _):
        out = receive_body(search, 2, p, 1)
        total = None
        for i, v in enumerate(out):
            field_b[p, i] = v
            total = v * v if total is None else total + v * v
        sums[PAIRS + p] = total
        send_time(unflat(out, 4), 3, p, -1, held=True)
        send_edges(unflat(out, 4), 3, p, -1)
        return _

    run(fourth, 0, PAIRS)

    def normal_of(p, _):
        give(normal_ref, p, receive_body(field_b, 3, p, -1))
        return _

    mine = jnp.zeros((8, 128), jnp.float32)
    for k in range(2 * PAIRS):
        mine = jnp.where(sh.lane == k, jnp.sum(sums[k], axis=1, keepdims=True), mine)
    slot = 0
    for stage, axis in enumerate(AXES):
        red_out[stage] = mine
        others = n_of[axis] - 1

        def sum_copy(k, place):
            return pltpu.make_async_remote_copy(
                src_ref=red_out.at[stage], dst_ref=red_in.at[place],
                send_sem=send_sem.at[4], recv_sem=red_sem.at[stage],
                device_id=peer(axis, k), device_id_type=MESH,
            )

        for k in range(1, others + 1):
            sum_copy(k, slot + k - 1).start()
        if stage == 0:
            interior(field_b, -1)
        if stage == 2:
            pl.when(first_core)(lambda: start_time(3, PAIRS - 1))
            run(normal_of, 0, PAIRS - 3)
            pl.when(other_core)(lambda: start_time(3, PAIRS - 2))
            run(normal_of, PAIRS - 3, PAIRS - 2)
            pl.when(other_core)(lambda: start_time(3, PAIRS - 1))
            run(normal_of, PAIRS - 2, PAIRS - 1)
        landed = red_in.at[pl.ds(slot, others)]
        pltpu.make_async_remote_copy(
            src_ref=landed, dst_ref=landed, send_sem=send_sem.at[4], recv_sem=red_sem.at[stage],
            device_id=peer(axis, 1), device_id_type=MESH,
        ).wait_recv()
        for k in range(others):
            mine = mine + red_in[slot + k]
        slot += others
    top = jnp.sum(mine[0:4], axis=0, keepdims=True)
    bottom = jnp.sum(mine[4:8], axis=0, keepdims=True)
    both = jnp.where(sh.low, top, bottom)
    curvature = pltpu.roll(both, 128 - PAIRS, 1)
    steps = both / jnp.where(sh.lane < PAIRS, curvature, 1.0)

    for p in range(PAIRS):
        length = jnp.sum(jnp.where(sh.lane == p, steps, 0.0), axis=1, keepdims=True)
        first = 6 * (p % 2) + p // 2
        second_rhs = first + 3
        length_ref[first : first + 1] = jnp.broadcast_to(length[0:1], (1, 128))
        length_ref[second_rhs : second_rhs + 1] = jnp.broadcast_to(length[4:5], (1, 128))

    run(normal_of, PAIRS - 1, PAIRS)

    passed = blocks.at[pl.ds(0, reach * n_gz - 1)]
    for k, (sent, landed) in enumerate((
        (edge_out, edge_in), (time_out, time_in), (passed, passed), (smt_out, smt_in), (red_in, red_in),
    )):
        pltpu.make_async_remote_copy(
            src_ref=sent, dst_ref=landed, send_sem=send_sem.at[k], recv_sem=red_sem.at[0],
            device_id=peer("ta", 1), device_id_type=MESH,
        ).wait_send()


def on_device(sizes, links, guess, source_sites):
    rows, lanes = guess.shape[-2:]
    f32 = jnp.float32
    copies = sum(n - 1 for n in sizes)
    n_gz = sizes[AXES.index("gz")]
    reach = min(sizes[0], 8)
    groups = reach // 2
    tile = (8, lanes)
    vm = lambda *shape: pltpu.VMEM(shape + tile, f32)
    dma = lambda *shape: pltpu.SemaphoreType.DMA(shape)
    out = jax.ShapeDtypeStruct((12, 12, 2 * rows, lanes), f32)
    search, normal, length = pl.pallas_call(
        functools.partial(kernel, sizes),
        out_shape=(out, out, jax.ShapeDtypeStruct((12, lanes), f32)),
        in_specs=[
            pl.BlockSpec(memory_space=pltpu.HBM),
            pl.BlockSpec(memory_space=pltpu.HBM),
            pl.BlockSpec(memory_space=pltpu.HBM),
        ],
        out_specs=(pl.BlockSpec(memory_space=pltpu.VMEM),) * 3,
        scratch_shapes=[
            pltpu.SMEM((4,), jnp.int32), pltpu.VMEM((72, rows, lanes), f32), pltpu.VMEM((12, 24, rows, lanes), f32),
            pltpu.VMEM((reach * n_gz, 55, rows, lanes), f32), vm(groups, n_gz, 55),
            vm(2, groups, n_gz, 18), vm(min(groups, 2), 2, groups, n_gz, 18),
            vm(72), vm(PAIRS, 24), vm(PAIRS, 24), vm(PAIRS, 24), vm(PAIRS, 24), vm(PAIRS, 24),
            vm(PAIRS, 24), vm(2, PAIRS, 12),
            vm(4, 4, PAIRS, 3), vm(4, 4, PAIRS, 3), vm(4, 2, PAIRS, 12), vm(4, 2, PAIRS, 12),
            vm(2, 3), vm(2, 3),
            vm(3), vm(copies), vm(2 * PAIRS), vm(5, 6), vm(3, 6),
            dma(4), dma(2, PAIRS // EDGE_CHUNK), dma(2, PAIRS), dma(reach * n_gz), dma(1), dma(3), dma(5),
        ],
        compiler_params=pltpu.CompilerParams(
            collective_id=0, has_side_effects=True, vmem_limit_bytes=48 * 1024 * 1024
        ),
    )(*(
        pltpu.with_memory_space_constraint(x, pltpu.HBM)
        for x in (
            source_sites.reshape(4), links.reshape(72, rows, lanes), guess.reshape(12, 24, rows, lanes)
        )
    ))
    length = length[:, None, None]
    sol = guess.reshape(search.shape) + length * search
    res = search - length * normal
    return sol.reshape(guess.shape), res.reshape(guess.shape)


def solution(mesh):
    sizes = tuple(mesh.shape[axis] for axis in AXES)
    fields = P(None, None, None, None, "ta", "xy", "gz")
    return jax.shard_map(
        functools.partial(on_device, sizes),
        mesh=mesh,
        in_specs=(fields, fields, P("ta", "xy", "gz", None)),
        out_specs=(fields, fields),
        check_vma=False,
    )
```
